256 devices in a mesh: vocab: 32 (over z_hi, x, y), batch: 8 (over z_lo, core).
Axes of the slice: x: 4, y: 4, z: 8 (z_hi: 2, z_lo: 4; z = z_hi * 4 + z_lo), core: 2. Of those that a mesh axis runs over, the one named last changes fastest.
Arguments:
- draft_hidden: bfloat16 [128, 4096], P('vocab', 'batch')
- target_hidden: bfloat16 [128, 8192], P('vocab', 'batch')
- draft_gain: float32 [4096], P('batch'), may hold values from 0.5 to 1.5
- target_gain: float32 [8192], P('batch'), may hold values from 0.5 to 1.5
- draft_head: bfloat16 [4096, 128256], P('batch', 'vocab')
- target_head: bfloat16 [8192, 128256], P('batch', 'vocab')
- token_class: int32 [128256], P('vocab'), may hold values from 0 to 29
- grammar_bits: int32 [128], replicated, may hold values from 0 to 1073741823
- draft_tokens: int32 [128], replicated, may hold values from 0 to 128255
Outputs:
- log_ratio: float32 [128], P('batch')
- target_logprob: float32 [128], P('batch')
The draws below stay inside these ranges and needn't reach their ends.
Inputs may be any that keep to these rules, and one draw needn't show every extreme that they name: `token_class`: a class number of 0 to 29 for each vocabulary entry. `grammar_bits`: bits 0 to 29 in use.
All inputs are finite; a program needn't handle non-finite values.
Results may differ from the reference program's by a relative error of at most 0.00042.
Values may be sent and summed in bfloat16 or wider, within the bound.
A program may use at most 64 MiB of HBM per device.

```python
import math
import jax
import jax.numpy as jnp
import numpy as np
from jax import lax

D_DRAFT = 4096
D_TARGET = 8192
VOCAB = 128256
CLASSES = 30
ROWS = 128


def strong_columns(key, offset_tag, feature_count):
    indices = jax.random.permutation(jax.random.fold_in(key, offset_tag), VOCAB)[:8]
    basis = jax.random.normal(jax.random.fold_in(key, offset_tag + 1), (8, feature_count), jnp.float32) * 300.0 / feature_count
    leading = basis[0::2]
    second = basis[1::2]
    second = second - jnp.sum(leading * second, axis=1, keepdims=True) / jnp.sum(leading * leading, axis=1, keepdims=True) * leading
    second = second * jnp.sqrt(jnp.sum(leading * leading, axis=1, keepdims=True) / jnp.sum(second * second, axis=1, keepdims=True))
    return (indices, leading, second)


def head_matrix(key, offset_tag, feature_count):
    indices, leading, second = strong_columns(key, offset_tag, feature_count)
    matrix = jax.random.normal(jax.random.fold_in(key, offset_tag + 2), (feature_count, VOCAB), jnp.float32) * 3.0 / math.sqrt(feature_count)
    stacked = jnp.stack([leading, second], axis=1).reshape(8, feature_count)
    matrix = matrix.at[:, indices].set(stacked.T)
    return matrix.astype(jnp.bfloat16)


def hidden_rows(key, offset_tag, feature_count):
    indices, leading, second = strong_columns(key, offset_tag, feature_count)
    position = jnp.arange(feature_count, dtype=jnp.float32) / max(feature_count - 1, 1)
    rising = jnp.exp(position * math.log(1.8))
    states = jax.random.normal(jax.random.fold_in(key, offset_tag + 3), (ROWS, feature_count), jnp.float32) * rising[None, :]
    strengths = jnp.array([0.0, 0.2, 0.4, 0.6], jnp.float32)
    noise = jax.random.normal(jax.random.fold_in(key, offset_tag + 4), (16, feature_count), jnp.float32) * 300.0 / feature_count
    counter = jnp.arange(16)
    pairing = counter % 4
    mixing = strengths[counter // 4]
    aligned = leading[pairing] + 0.993 * second[pairing] + mixing[:, None] * noise
    states = states.at[counter * (ROWS // 16)].set(aligned)
    return states.astype(jnp.bfloat16)


def draw_draft_head(key, part):
    return head_matrix(key, 100, D_DRAFT)


def draw_target_head(key, part):
    return head_matrix(key, 200, D_TARGET)


def draw_draft_hidden(key, part):
    return hidden_rows(key, 100, D_DRAFT)


def draw_target_hidden(key, part):
    return hidden_rows(key, 200, D_TARGET)


def with_ends(drawn, stream_key, least, high):
    longest = drawn.shape.index(max(drawn.shape))
    spots = []
    for shift in (0, 1):
        where = [jax.random.randint(jax.random.fold_in(stream_key, axis), (), 0, length) for axis, length in enumerate(drawn.shape)]
        where[longest] = (where[longest] + shift) % drawn.shape[longest]
        spots.append(tuple(where))
    return drawn.at[spots[0]].set(least).at[spots[1]].set(high)


def wide_ids(rng, shape, amount, slope):
    weights = [min(1 << octave, amount + 1 - (1 << octave)) * (1 << 20) // math.isqrt((1 << octave) ** slope) + 1 for octave in range((amount + 1).bit_length()) if 1 << octave <= amount]
    scale = 1 + sum(weights) // (1 << 30)
    listing = np.cumsum(np.array([max(1, weight // scale) for weight in weights]))
    lot = jax.random.randint(jax.random.fold_in(rng, 1), shape, 0, int(listing[len(weights) - 1]))
    start = jnp.left_shift(1, jnp.searchsorted(jnp.asarray(listing, jnp.int32), lot, side="right").astype(jnp.int32))
    standing = start - 1 + jax.random.randint(jax.random.fold_in(rng, 4), shape, 0, 1 << 30) % jnp.minimum(start, amount + 1 - start)
    return jax.random.permutation(jax.random.fold_in(rng, 2), amount)[standing].astype(jnp.int32)


def setup_inputs(seed: int = 0) -> dict:
    key_of = jax.random.split(jax.random.key(seed), 10)
    return {
        "draft_hidden": draw_draft_hidden(jax.random.fold_in(key_of[9], 71), 0),
        "target_hidden": draw_target_hidden(jax.random.fold_in(key_of[9], 71), 0),
        "draft_gain": jnp.clip(1.0 + 0.1 * jax.random.normal(key_of[2], (D_DRAFT,), jnp.float32), 0.5, 1.5),
        "target_gain": jnp.clip(1.0 + 0.1 * jax.random.normal(key_of[3], (D_TARGET,), jnp.float32), 0.5, 1.5),
        "draft_head": draw_draft_head(jax.random.fold_in(key_of[9], 71), 0),
        "target_head": draw_target_head(jax.random.fold_in(key_of[9], 71), 0),
        "token_class": with_ends(jax.random.randint(key_of[6], (VOCAB,), 0, CLASSES), jax.random.fold_in(key_of[6], 1), 0, CLASSES - 1).astype(jnp.int32),
        "grammar_bits": with_ends(jax.random.randint(key_of[7], (ROWS,), 0, 2 ** 30), jax.random.fold_in(key_of[7], 1), 0, (2 ** 30) - 1).astype(jnp.int32),
        "draft_tokens": with_ends(wide_ids(key_of[8], (ROWS,), VOCAB, 2), jax.random.fold_in(key_of[8], 3), 0, VOCAB - 1).astype(jnp.int32),
    }


eps_norm = 1e-05
neg_fill = -1e+30

def final_norm(hidden, gain_vec):
    values = hidden.astype(jnp.float32)
    scale = lax.rsqrt(lax.optimization_barrier(jnp.mean(values * values, axis=1, keepdims=True)) + eps_norm)
    return (values * scale * gain_vec.astype(jnp.float32)[None, :]).astype(jnp.bfloat16)

def masked_parts(logits, allowed, chosen):
    masked = jnp.where(allowed, logits, neg_fill)
    highest = lax.optimization_barrier(jnp.max(masked, axis=1))
    summed = lax.optimization_barrier(jnp.sum(jnp.where(allowed, jnp.exp(masked - highest[:, None]), 0.0), axis=1))
    picked = lax.optimization_barrier(jnp.sum(jnp.where(chosen, logits, 0.0), axis=1))
    return (highest + jnp.log(summed), picked)

def reference(draft_hidden, target_hidden, draft_gain, target_gain, draft_head, target_head, token_class, grammar_bits, draft_tokens):
    columns = lax.broadcasted_iota(jnp.int32, (1, VOCAB), 1)
    chosen = columns == draft_tokens.astype(jnp.int32)[:, None]
    bit_on = grammar_bits[:, None] >> token_class[None, :] & 1 == 1
    allowed = bit_on | chosen
    draft_logits = jnp.dot(final_norm(draft_hidden, draft_gain), draft_head, preferred_element_type=jnp.float32)
    draft_lse, draft_pick = masked_parts(draft_logits, allowed, chosen)
    target_logits = jnp.dot(final_norm(target_hidden, target_gain), target_head, preferred_element_type=jnp.float32)
    target_lse, target_pick = masked_parts(target_logits, allowed, chosen)
    target_logprob = target_pick - target_lse
    log_ratio = target_logprob - (draft_pick - draft_lse)
    return (log_ratio, target_logprob)
```

```python
import functools
import math

import jax
import jax.numpy as jnp
from jax import lax
from jax.experimental import pallas as pl
from jax.experimental.pallas import tpu as pltpu
from jax.sharding import PartitionSpec as P

D_DRAFT = 4096
D_TARGET = 8192
EPS = 1e-05
NEG = -1e30
F32 = jnp.float32
BF16 = jnp.bfloat16

PLANE = 16
CHAIN = 4
ROWS = 128
HALF = 64
BLOCK = 16
CW = 1024
Q = 4
PER_STAGE = 2 * Q
CHUNKS = 2 * PER_STAGE
LAG = 1
HOP = 3
WSPLIT = 1024
LEVELS = 32760.0


def kernel(
    dims,
    dh, th, dg, tg, wd_hbm, wt_hbm, cls_hbm, bits_hbm, tok_hbm,
    ratio_ref, logprob_ref,
    xg, gain, wd, wt, cls_in, cls, colid, bits_s, tok_s,
    xf, xn, srow, ssib, pb, pr, sb, rb, qs, qr, hs, hr, fb, bt, st,
    grow, gall, zrow, zall,
    load_sem, w_sem, near_send, far_send, pair_send, g_recv,
    d2_send, d2_recv, sib_send, sib_recv,
    c_send, c_recv, q_send, q_recv, h_send, h_recv,
    fin_send, fin_recv, z_send, z_recv,
):
    kd, kt, width = dims
    kk = kd + kt
    v = lax.axis_index("vocab")
    b = lax.axis_index("batch")
    half = v // PLANE
    place = v % PLANE
    chip = b // 2
    core = b % 2
    mate = chip * 2 + (1 - core)
    partner = (v + PLANE) % (2 * PLANE)

    def remote(src, dst, send, recv, vv, bb):
        return pltpu.make_async_remote_copy(
            src_ref=src, dst_ref=dst, send_sem=send, recv_sem=recv,
            device_id=(vv, bb), device_id_type=pl.DeviceIdType.MESH,
        )

    loads = [
        pltpu.make_async_copy(dh, xg.at[v, :, 0:kd], load_sem.at[0]),
        pltpu.make_async_copy(th, xg.at[v, :, kd:kk], load_sem.at[1]),
        pltpu.make_async_copy(dg, gain.at[:, 0:kd], load_sem.at[2]),
        pltpu.make_async_copy(tg, gain.at[:, kd:kk], load_sem.at[3]),
        pltpu.make_async_copy(cls_hbm, cls_in, load_sem.at[4]),
        pltpu.make_async_copy(bits_hbm, bits_s, load_sem.at[5]),
        pltpu.make_async_copy(tok_hbm, tok_s, load_sem.at[6]),
    ]
    for copy in loads:
        copy.start()

    barrier = pltpu.get_barrier_semaphore()

    def greet(vv, bb):
        pl.semaphore_signal(
            barrier, inc=1, device_id=(vv, bb), device_id_type=pl.DeviceIdType.MESH
        )

    def greet_plane(t, carry):
        greet(half * PLANE + (place + t) % PLANE, b)
        return carry

    def greet_line(t, carry):
        zz = (half * CHAIN + chip + t) % (2 * CHAIN)
        greet((zz // CHAIN) * PLANE + place, (zz % CHAIN) * 2 + core)
        return carry

    lax.fori_loop(1, 2 * CHAIN, greet_line, 0)
    lax.fori_loop(1, PLANE, greet_plane, 0)
    greet(v, mate)

    weights = []
    for hbm, ref in ((wd_hbm, wd), (wt_hbm, wt)):
        for at in range(0, width, WSPLIT):
            rows = pl.ds(at, min(WSPLIT, width - at))
            weights.append((hbm.at[rows], ref.at[rows]))
    weights = [
        pltpu.make_async_copy(src, dst, w_sem.at[n]) for n, (src, dst) in enumerate(weights)
    ]
    for copy in weights:
        copy.start()

    pl.semaphore_wait(barrier, (2 * CHAIN - 1) + (PLANE - 1) + 1)

    loads[0].wait()
    loads[1].wait()
    to_partner = remote(xg.at[v], xg.at[v], pair_send.at[0], g_recv.at[v], partner, b)
    to_partner.start()

    def near_copy(t):
        return remote(
            xg.at[v], xg.at[v], near_send.at[t], g_recv.at[v],
            half * PLANE + (place + t) % PLANE, b,
        )

    def far_copy(t):
        return remote(
            xg.at[partner], xg.at[partner], far_send.at[t], g_recv.at[partner],
            half * PLANE + (place + t) % PLANE, b,
        )

    def arrived(vv):
        remote(xg.at[vv], xg.at[vv], pair_send.at[0], g_recv.at[vv], v, b).wait_recv()

    def start_near(t, carry):
        near_copy(t).start()
        return carry

    def start_far(t, carry):
        far_copy(t).start()
        return carry

    lax.fori_loop(1, PLANE, start_near, 0)

    for copy in loads[2:]:
        copy.wait()
    lanes_all = lax.broadcasted_iota(jnp.int32, (1, Q * CW), 1)
    colid[...] = jnp.where(lanes_all < width, lanes_all, -(1 << 30))
    cls[...] = jnp.full((1, Q * CW), 30, jnp.int32)
    cls[:, 0:width] = cls_in[...]
    lane = lax.broadcasted_iota(jnp.int32, (BLOCK, 128), 1)
    sub = lax.broadcasted_iota(jnp.int32, (BLOCK, 128), 0)
    for a in range(2):
        stage = half if a == 0 else 1 - half
        at = (stage * 4 + (chip // 2) * 2 + core) * BLOCK
        bits_col = jnp.zeros((BLOCK, 128), jnp.int32)
        tok_col = jnp.zeros((BLOCK, 128), jnp.int32)
        for r in range(BLOCK):
            bits_col = jnp.where(sub == r, bits_s[at + r], bits_col)
            tok_col = jnp.where(sub == r, tok_s[at + r], tok_col)
        bt[a, 0] = bits_col
        bt[a, 1] = tok_col - v * width
        for m in range(2):
            st[a * 2 + m, 0] = jnp.full((BLOCK, 128), NEG, F32)
            st[a * 2 + m, 1] = jnp.zeros((BLOCK, 128), F32)
            st[a * 2 + m, 2] = jnp.zeros((BLOCK, 128), F32)
    for d in range(2):
        pos = chip if d else (CHAIN - 1) - chip

        @pl.when(pos == 0)
        def _():
            hr[d] = jnp.zeros((2, 1, 128), F32)

    for copy in weights:
        copy.wait()
    wd[width:, :] = jnp.zeros((Q * CW - width, kd), BF16)
    wt[width:, :] = jnp.zeros((Q * CW - width, kt), BF16)

    arrived(partner)
    lax.fori_loop(1, PLANE, start_far, 0)

    def prepare(a):
        stage = half if a == 0 else 1 - half

        def wait_row(t, carry):
            arrived(stage * PLANE + (place + t) % PLANE)
            return carry

        lax.fori_loop(1, PLANE, wait_row, 0)
        for i in range(PLANE):
            xf[4 * i : 4 * i + 4, :] = xg[stage * PLANE + i].astype(F32)
        gv = gain[...]
        total = jnp.zeros((BLOCK, 128), F32)
        for g in range(HALF // BLOCK):
            values = xf[g * BLOCK : (g + 1) * BLOCK, :]
            for m, (lo, hi) in enumerate(((0, kd), (kd, kk))):
                part = values[:, lo:hi]
                square = jnp.sum(part * part, axis=1, keepdims=True) + (hi - lo) * EPS
                scaled = part * lax.rsqrt(square) * gv[:, lo:hi]
                xn[a, g * BLOCK : (g + 1) * BLOCK, lo:hi] = scaled.astype(BF16)
                total = total + jnp.where(lane == sub + (m * HALF + g * BLOCK), square, 0.0)
        srow[a] = jnp.sum(total, axis=0, keepdims=True)
        remote(srow.at[a], ssib.at[a], sib_send.at[a], sib_recv.at[a], v, mate).start()

    def multiply(s):
        a = s // PER_STAGE
        r = s % PER_STAGE
        quarter = r // 2

        def run(ref, lo, hi):
            left = xn[a, :, lo:hi]
            for n in range(CW // 256):
                at = pl.multiple_of(quarter * CW + n * 256, 256)
                out = lax.dot_general(
                    left, ref[pl.ds(at, 256), :], (((1,), (1,)), ((), ())),
                    preferred_element_type=F32,
                )
                for blk in range(HALF // BLOCK):
                    pb[s, blk % 2, blk // 2, :, n * 256 : (n + 1) * 256] = out[
                        blk * BLOCK : (blk + 1) * BLOCK
                    ]

        @pl.when(r % 2 == 0)
        def _():
            run(wd, 0, kd)

        @pl.when(r % 2 == 1)
        def _():
            run(wt, kd, kk)

    def d2_copy(j):
        return remote(pb.at[j, 1 - core], pr.at[j], d2_send.at[j], d2_recv.at[j], v, mate)

    def chain_to(d):
        return (chip + (1 if d else -1)) * 2 + core

    def chunk_copy(d, j):
        return remote(sb.at[d, j], rb.at[d, j], c_send.at[d, j], c_recv.at[d, j], v, chain_to(d))

    def scale_copy(d, j):
        return remote(qs.at[d, j], qr.at[d, j], q_send.at[d, j], q_recv.at[d, j], v, chain_to(d))

    def head_copy(d, a):
        return remote(hs.at[d, a], hr.at[d, a], h_send.at[d, a], h_recv.at[d, a], v, chain_to(d))

    def head(d, a, pos):
        @pl.when(pos > 0)
        def _():
            head_copy(d, a).wait_recv()

        own, sib, up = srow[a], ssib[a], hr[d, a]
        new = own + sib + up
        hs[d, a] = new

        @pl.when(pos < CHAIN - 1)
        def _():
            head_copy(d, a).start()

        inverse = 1.0 / new
        factors = [jnp.sqrt(part * inverse) for part in (own, sib, up)]
        for m, depth in enumerate((D_DRAFT, D_TARGET)):
            grow_by = jnp.where(pos == CHAIN - 1, math.sqrt(depth), 1.0)
            pick = lane == sub + (m * HALF + d * 2 * BLOCK) + core * BLOCK
            for n, factor in enumerate(factors):
                column = jnp.sum(jnp.where(pick, factor, 0.0), axis=1, keepdims=True)
                fb[d, a, m, n] = jnp.broadcast_to(column * grow_by, (BLOCK, 128))

    def chain(d, s):
        pos = chip if d else (CHAIN - 1) - chip
        j = s - LAG - pos * HOP
        groups = CW // 128

        def cut(g):
            return slice(g * 128, (g + 1) * 128)

        @pl.when((j >= 0) & (j < CHUNKS))
        def _():
            a = j // PER_STAGE
            r = j % PER_STAGE
            m = r % 2

            @pl.when(r == 0)
            def _():
                head(d, a, pos)

            def local_sum():
                fo, fs = fb[d, a, m, 0], fb[d, a, m, 1]
                return [
                    pb[j, core, d, :, cut(g)] * fo + pr[j, d, :, cut(g)] * fs
                    for g in range(groups)
                ]

            def with_received():
                chunk_copy(d, j).wait_recv()
                scale_copy(d, j).wait_recv()
                fu = fb[d, a, m, 2] * qr[d, j]
                return [
                    part + rb[d, j, :, cut(g)].astype(F32) * fu
                    for g, part in enumerate(local_sum())
                ]

            def send(parts):
                top = functools.reduce(jnp.maximum, [jnp.abs(p) for p in parts])
                top = jnp.maximum(jnp.max(top, axis=0, keepdims=True), 1e-30)
                up = LEVELS / top
                qs[d, j] = top * (1.0 / LEVELS)
                for g, part in enumerate(parts):
                    sb[d, j, :, cut(g)] = (
                        jnp.round(part * up).astype(jnp.int32).astype(jnp.int16)
                    )
                scale_copy(d, j).start()
                chunk_copy(d, j).start()

            @pl.when(pos == 0)
            def _():
                send(local_sum())

            @pl.when((pos > 0) & (pos < CHAIN - 1))
            def _():
                send(with_received())

            @pl.when(pos == CHAIN - 1)
            def _():
                logits = with_received()
                base = (r // 2) * CW
                bits, tok = bt[a, 0], bt[a, 1]
                at = a * 2 + m
                high, summed, picked = st[at, 0], st[at, 1], st[at, 2]
                masked, keeps = [], []
                for g in range(groups):
                    off = pl.ds(pl.multiple_of(base + g * 128, 128), 128)
                    chosen = colid[:, off] == tok
                    keep = ((bits >> cls[:, off]) & 1 == 1) | chosen
                    picked = picked + jnp.where(chosen, logits[g], 0.0)
                    masked.append(jnp.where(keep, logits[g], NEG))
                    keeps.append(keep)
                top = functools.reduce(jnp.maximum, masked, high)
                summed = summed * jnp.exp(high - top)
                for g in range(groups):
                    summed = summed + jnp.where(keeps[g], jnp.exp(masked[g] - top), 0.0)
                st[at, 0] = top
                st[at, 1] = summed
                st[at, 2] = picked

    def slot(s, carry):
        @pl.when(s == 0)
        def _():
            prepare(0)

        @pl.when(s == PER_STAGE)
        def _():
            prepare(1)

        @pl.when(s < CHUNKS)
        def _():
            multiply(s)
            d2_copy(s).start()

        late = s - LAG

        @pl.when((late >= 0) & (late < CHUNKS))
        def _():
            d2_copy(late).wait_recv()

            @pl.when(late % PER_STAGE == 0)
            def _():
                a = late // PER_STAGE
                remote(
                    srow.at[a], ssib.at[a], sib_send.at[a], sib_recv.at[a], v, mate
                ).wait_recv()

        chain(1, s)
        chain(0, s)
        return carry

    lax.fori_loop(0, CHUNKS + LAG + (CHAIN - 1) * HOP, slot, 0)

    owner = (chip == 0) | (chip == CHAIN - 1)
    lane1 = lax.broadcasted_iota(jnp.int32, (1, 128), 1)

    def merge(rows):
        sums = jnp.sum(rows, axis=0, keepdims=True)
        top = jnp.max(rows, axis=0, keepdims=True)
        lse = top + jnp.log(jnp.sum(jnp.exp(rows - top), axis=0, keepdims=True))
        return jnp.where(lane1 < 64, lse, sums)

    def fin_copy(t):
        return remote(
            grow.at[0], gall.at[place], fin_send.at[t], fin_recv.at[place],
            half * PLANE + (place + t) % PLANE, b,
        )

    def z_copy(n):
        hh = (half + n % 2) % 2
        end = chip // 2
        low = end * 3
        other = 2 - end
        target = low if n < 2 else other
        return remote(
            zrow.at[0], zall.at[half], z_send.at[n], z_recv.at[half],
            hh * PLANE + place, target * 2 + core,
        )

    def z_arrived(hh):
        remote(
            zrow.at[0], zall.at[hh], z_send.at[0], z_recv.at[hh], v, b
        ).wait_recv()

    @pl.when(owner)
    def _():
        total = jnp.zeros((BLOCK, 128), F32)
        for a in range(2):
            stage = half if a == 0 else 1 - half
            for m in range(2):
                high, summed, picked = (st[a * 2 + m, n] for n in range(3))
                top = jnp.max(high, axis=1, keepdims=True)
                mass = jnp.sum(summed * jnp.exp(high - top), axis=1, keepdims=True)
                lse = jnp.where(mass > 0.0, top + jnp.log(jnp.maximum(mass, 1e-37)), NEG)
                pick = jnp.sum(picked, axis=1, keepdims=True)
                at = sub + stage * BLOCK + m * 32
                total = total + jnp.where(lane == at, lse, 0.0)
                total = total + jnp.where(lane == at + 64, pick, 0.0)
        row = jnp.sum(total, axis=0, keepdims=True)
        grow[0] = row
        gall[place] = row

        def start(t, carry):
            fin_copy(t).start()
            return carry

        lax.fori_loop(1, PLANE, start, 0)

        def wait(t, carry):
            n = (place + t) % PLANE
            remote(
                grow.at[0], gall.at[n], fin_send.at[t], fin_recv.at[n], v, b
            ).wait_recv()
            return carry

        lax.fori_loop(1, PLANE, wait, 0)
        row = merge(gall[...].reshape(PLANE, 128))
        zrow[0] = row
        zall[half] = row
        for n in (3, 2, 1):
            z_copy(n).start()
        z_arrived(1 - half)

    @pl.when(jnp.logical_not(owner))
    def _():
        z_arrived(0)
        z_arrived(1)

    row = merge(zall[...].reshape(2, 128))
    stage = chip // 2

    def part(n):
        return jnp.where(
            stage == 0, row[:, n * 32 : n * 32 + 16], row[:, n * 32 + 16 : n * 32 + 32]
        )

    logprob = part(3) - part(1)
    logprob_ref[...] = logprob
    ratio_ref[...] = logprob - (part(2) - part(0))

    to_partner.wait_send()

    def drain_gather(t, carry):
        near_copy(t).wait_send()
        far_copy(t).wait_send()
        return carry

    lax.fori_loop(1, PLANE, drain_gather, 0)
    for a in range(2):
        remote(srow.at[a], ssib.at[a], sib_send.at[a], sib_recv.at[a], v, mate).wait_send()

    def drain_chunks(j, carry):
        d2_copy(j).wait_send()
        return carry

    lax.fori_loop(0, CHUNKS, drain_chunks, 0)
    for d in range(2):
        pos = chip if d else (CHAIN - 1) - chip

        @pl.when(pos < CHAIN - 1)
        def _():
            for a in range(2):
                head_copy(d, a).wait_send()

            def drain_chain(j, carry):
                chunk_copy(d, j).wait_send()
                scale_copy(d, j).wait_send()
                return carry

            lax.fori_loop(0, CHUNKS, drain_chain, 0)

    @pl.when(owner)
    def _():
        def drain_final(t, carry):
            fin_copy(t).wait_send()
            return carry

        lax.fori_loop(1, PLANE, drain_final, 0)
        for n in (3, 2, 1):
            z_copy(n).wait_send()


def shards(
    draft_hidden, target_hidden, draft_gain, target_gain, draft_head, target_head,
    token_class, grammar_bits, draft_tokens,
):
    kd, width = draft_head.shape
    kt = target_head.shape[0]
    kk = kd + kt
    vmem, dma = pltpu.VMEM, pltpu.SemaphoreType.DMA
    i32, i16 = jnp.int32, jnp.int16
    scratch = [
        vmem((2 * PLANE, 4, kk), BF16),
        vmem((1, kk), F32),
        vmem((Q * CW, kd), BF16),
        vmem((Q * CW, kt), BF16),
        vmem((1, width), i32),
        vmem((1, Q * CW), i32),
        vmem((1, Q * CW), i32),
        pltpu.SMEM((ROWS,), i32),
        pltpu.SMEM((ROWS,), i32),
        vmem((HALF, kk), F32),
        vmem((2, HALF, kk), BF16),
        vmem((2, 1, 128), F32),
        vmem((2, 1, 128), F32),
        vmem((CHUNKS, 2, 2, BLOCK, CW), F32),
        vmem((CHUNKS, 2, BLOCK, CW), F32),
        vmem((2, CHUNKS, BLOCK, CW), i16),
        vmem((2, CHUNKS, BLOCK, CW), i16),
        vmem((2, CHUNKS, 1, 128), F32),
        vmem((2, CHUNKS, 1, 128), F32),
        vmem((2, 2, 1, 128), F32),
        vmem((2, 2, 1, 128), F32),
        vmem((2, 2, 2, 3, BLOCK, 128), F32),
        vmem((2, 2, BLOCK, 128), i32),
        vmem((4, 3, BLOCK, 128), F32),
        vmem((1, 1, 128), F32),
        vmem((PLANE, 1, 128), F32),
        vmem((1, 1, 128), F32),
        vmem((2, 1, 128), F32),
        dma((7,)),
        dma((2 * pl.cdiv(width, WSPLIT),)),
        dma((PLANE,)),
        dma((PLANE,)),
        dma((1,)),
        dma((2 * PLANE,)),
        dma((CHUNKS,)),
        dma((CHUNKS,)),
        dma((2,)),
        dma((2,)),
        dma((2, CHUNKS)),
        dma((2, CHUNKS)),
        dma((2, CHUNKS)),
        dma((2, CHUNKS)),
        dma((2, 2)),
        dma((2, 2)),
        dma((PLANE,)),
        dma((PLANE,)),
        dma((4,)),
        dma((2,)),
    ]
    out = jax.ShapeDtypeStruct((1, BLOCK), F32)
    ratio, logprob = pl.pallas_call(
        functools.partial(kernel, (kd, kt, width)),
        out_shape=(out, out),
        in_specs=[pl.BlockSpec(memory_space=pl.ANY)] * 9,
        out_specs=(pl.BlockSpec(memory_space=pltpu.VMEM),) * 2,
        scratch_shapes=scratch,
        compiler_params=pltpu.CompilerParams(
            collective_id=0, has_side_effects=True, vmem_limit_bytes=62 * 1024 * 1024
        ),
        name="verify",
    )(
        draft_hidden,
        target_hidden,
        draft_gain.reshape(1, kd),
        target_gain.reshape(1, kt),
        draft_head.T,
        target_head.T,
        token_class.reshape(1, width),
        grammar_bits,
        draft_tokens,
    )
    return ratio.reshape(BLOCK), logprob.reshape(BLOCK)


def solution(mesh):
    in_specs = (
        P("vocab", "batch"),
        P("vocab", "batch"),
        P("batch"),
        P("batch"),
        P("batch", "vocab"),
        P("batch", "vocab"),
        P("vocab"),
        P(),
        P(),
    )
    out_specs = (P("batch"), P("batch"))
    return jax.shard_map(shards, mesh=mesh, in_specs=in_specs, out_specs=out_specs, check_vma=False)
```

```python
import functools

import jax
import jax.numpy as jnp
from jax import lax
from jax.experimental import pallas as pl
from jax.experimental.pallas import tpu as pltpu
from jax.sharding import PartitionSpec as P

D_DRAFT = 4096
D_TARGET = 8192
EPS = 1e-05
NEG = -1e30
F32 = jnp.float32
BF16 = jnp.bfloat16

PLANE = 16
CHAIN = 4
LINE = 16
ROWS = 128
SHARE = 4
BLOCK = 16
MINE = 32
CW = 256
CHUNKS = 16
LAG = 2
HOP = 4
WSPLIT = 1024
LEVELS = 32760.0


def kernel(
    dims,
    dh, th, dg, tg, wd_hbm, wt_hbm, cls_hbm, bits_hbm, tok_hbm,
    out_ref,
    own, other, gain, sums, xg, wd, wt, cls_in, cls, colid, bits_s, tok_s,
    xf, xn, pb, pr, sb, rb, qs, qr, bt, st,
    grow, gall, zrow, zall,
    load_sem, w_sem, sum_send, sum_recv, pair_send, pair_recv,
    near_send, far_send, g_recv, d2_send, d2_recv,
    c_send, c_recv, q_send, q_recv,
    fin_send, fin_recv, z_send, z_recv,
):
    kd, kt, width = dims
    kk = kd + kt
    v = lax.axis_index("vocab")
    b = lax.axis_index("batch")
    half = v // PLANE
    place = v % PLANE
    chip = b // 2
    core = b % 2
    mate = chip * 2 + (1 - core)
    partner = (v + PLANE) % (2 * PLANE)
    here = half * 8 + b

    def remote(src, dst, send, recv, vv, bb):
        return pltpu.make_async_remote_copy(
            src_ref=src, dst_ref=dst, send_sem=send, recv_sem=recv,
            device_id=(vv, bb), device_id_type=pl.DeviceIdType.MESH,
        )

    barrier = pltpu.get_barrier_semaphore()

    def greet(vv, bb):
        pl.semaphore_signal(
            barrier, inc=1, device_id=(vv, bb), device_id_type=pl.DeviceIdType.MESH
        )

    def greet_line(t, carry):
        to = (here + t) % LINE
        greet((to // 8) * PLANE + place, to % 8)
        return carry

    def greet_plane(t, carry):
        greet(half * PLANE + (place + t) % PLANE, b)
        return carry

    lax.fori_loop(1, LINE, greet_line, 0)
    lax.fori_loop(1, PLANE, greet_plane, 0)

    loads = [
        pltpu.make_async_copy(dh, own.at[:, 0:kd], load_sem.at[0]),
        pltpu.make_async_copy(th, own.at[:, kd:kk], load_sem.at[1]),
        pltpu.make_async_copy(dg, gain.at[:, 0:kd], load_sem.at[2]),
        pltpu.make_async_copy(tg, gain.at[:, kd:kk], load_sem.at[3]),
        pltpu.make_async_copy(cls_hbm, cls_in, load_sem.at[4]),
        pltpu.make_async_copy(bits_hbm, bits_s, load_sem.at[5]),
        pltpu.make_async_copy(tok_hbm, tok_s, load_sem.at[6]),
    ]
    for copy in loads:
        copy.start()
    weights = []
    for hbm, ref in ((wd_hbm, wd), (wt_hbm, wt)):
        for at in range(0, width, WSPLIT):
            rows = pl.ds(at, min(WSPLIT, width - at))
            weights.append((hbm.at[rows], ref.at[rows]))
    weights = [
        pltpu.make_async_copy(src, dst, w_sem.at[n]) for n, (src, dst) in enumerate(weights)
    ]
    for copy in weights:
        copy.start()

    lane4 = lax.broadcasted_iota(jnp.int32, (SHARE, 128), 1)
    sub4 = lax.broadcasted_iota(jnp.int32, (SHARE, 128), 0)
    models = ((0, kd, D_DRAFT), (kd, kk, D_TARGET))
    loads[0].wait()
    loads[1].wait()
    held = jnp.zeros((SHARE, 128), F32)
    for m, (lo, hi, _) in enumerate(models):
        part = own[:, lo:hi].astype(F32)
        square = jnp.sum(part * part, axis=1, keepdims=True)
        held = held + jnp.where(lane4 == sub4 + m * SHARE, square, 0.0)
    sums[here] = jnp.sum(held, axis=0, keepdims=True)

    pl.semaphore_wait(barrier, (LINE - 1) + (PLANE - 1))

    def pair_copy():
        return remote(own, other, pair_send.at[0], pair_recv.at[0], partner, b)

    def sum_copy(t):
        to = (here + t) % LINE
        return remote(
            sums.at[here], sums.at[here], sum_send.at[t], sum_recv.at[here],
            (to // 8) * PLANE + place, to % 8,
        )

    def sum_arrived(n):
        remote(sums.at[n], sums.at[n], sum_send.at[0], sum_recv.at[n], v, b).wait_recv()

    def start_sum(t, carry):
        sum_copy(t).start()
        return carry

    lax.fori_loop(1, LINE, start_sum, 0)
    pair_copy().start()

    for copy in loads[2:]:
        copy.wait()
    lane = lax.broadcasted_iota(jnp.int32, (MINE, 128), 1)
    sub = lax.broadcasted_iota(jnp.int32, (MINE, 128), 0)
    bits_col = jnp.zeros((MINE, 128), jnp.int32)
    tok_col = jnp.zeros((MINE, 128), jnp.int32)
    for stage in range(2):
        at = (stage * 4 + (chip // 2) * 2 + core) * BLOCK
        for r in range(BLOCK):
            row = sub == stage * BLOCK + r
            bits_col = jnp.where(row, bits_s[at + r], bits_col)
            tok_col = jnp.where(row, tok_s[at + r], tok_col)
    bt[0] = bits_col
    bt[1] = tok_col - v * width

    def normalise(rows, n, to):
        total = jnp.sum(sums[pl.ds(n * 8, 8)].reshape(8, 128), axis=0, keepdims=True)
        for m, (lo, hi, depth) in enumerate(models):
            column = jnp.sum(
                jnp.where(lane4 == sub4 + m * SHARE, total, 0.0), axis=1, keepdims=True
            )
            scale = lax.rsqrt(column / depth + EPS)
            xg[to, :, lo:hi] = (rows[:, lo:hi].astype(F32) * scale * gain[:, lo:hi]).astype(BF16)

    def near_copy(t):
        return remote(
            xg.at[v], xg.at[v], near_send.at[t], g_recv.at[v],
            half * PLANE + (place + t) % PLANE, b,
        )

    def far_copy(t):
        return remote(
            xg.at[partner], xg.at[partner], far_send.at[t], g_recv.at[partner],
            half * PLANE + (place + t) % PLANE, b,
        )

    def start_near(t, carry):
        near_copy(t).start()
        return carry

    def start_far(t, carry):
        far_copy(t).start()
        return carry

    def wait_same(t, carry):
        sum_arrived(half * 8 + (b + t) % 8)
        return carry

    def wait_opposite(t, carry):
        sum_arrived((1 - half) * 8 + t)
        return carry

    lax.fori_loop(1, 8, wait_same, 0)
    normalise(own, half, v)
    lax.fori_loop(1, PLANE, start_near, 0)
    lax.fori_loop(0, 8, wait_opposite, 0)
    pair_copy().wait_recv()
    normalise(other, 1 - half, partner)
    lax.fori_loop(1, PLANE, start_far, 0)

    lanes_all = lax.broadcasted_iota(jnp.int32, (1, CHUNKS * CW), 1)
    colid[...] = jnp.where(lanes_all < width, lanes_all, -(1 << 30))
    cls[...] = jnp.full((1, CHUNKS * CW), 30, jnp.int32)
    cls[:, 0:width] = cls_in[...]
    for m in range(2):
        st[m, 0] = jnp.full((MINE, 128), NEG, F32)
        st[m, 1] = jnp.zeros((MINE, 128), F32)
        st[m, 2] = jnp.zeros((MINE, 128), F32)
    for copy in weights:
        copy.wait()
    wd[width:, :] = jnp.zeros((CHUNKS * CW - width, kd), BF16)
    wt[width:, :] = jnp.zeros((CHUNKS * CW - width, kt), BF16)

    def settle(stage, first):
        def wait_row(t, carry):
            n = stage * PLANE + (place + t) % PLANE
            remote(xg.at[n], xg.at[n], near_send.at[0], g_recv.at[n], v, b).wait_recv()
            return carry

        lax.fori_loop(1, PLANE, wait_row, 0)

        def unpack(i, carry):
            for k in range(4):
                xf[i, 4 * k : 4 * k + 4, :] = xg[stage * PLANE + 4 * i + k].astype(F32)
            at = pl.multiple_of((stage * 4 + i) * BLOCK, BLOCK)
            xn[pl.ds(at, BLOCK), :] = xf[i].astype(BF16)
            return carry

        lax.fori_loop(0, 4, unpack, 0)

    settle(half, True)
    settle(1 - half, False)

    def multiply(s):
        for m, ref in enumerate((wd, wt)):
            lo, hi, _ = models[m]
            for n in range(CW // 256):
                at = pl.multiple_of(s * CW + n * 256, 256)
                out = lax.dot_general(
                    xn[:, lo:hi], ref[pl.ds(at, 256), :], (((1,), (1,)), ((), ())),
                    preferred_element_type=F32,
                )
                col = m * CW + n * 256
                for blk in range(ROWS // BLOCK):
                    row = (blk // 4) * BLOCK
                    pb[s, blk % 2, (blk // 2) % 2, row : row + BLOCK, col : col + 256] = out[
                        blk * BLOCK : (blk + 1) * BLOCK
                    ]

    def d2_copy(j):
        return remote(pb.at[j, 1 - core], pr.at[j], d2_send.at[j], d2_recv.at[j], v, mate)

    def chain_to(d):
        return (chip + (1 if d else -1)) * 2 + core

    def chunk_copy(d, j):
        return remote(sb.at[d, j], rb.at[d, j], c_send.at[d, j], c_recv.at[d, j], v, chain_to(d))

    def scale_copy(d, j):
        return remote(qs.at[d, j], qr.at[d, j], q_send.at[d, j], q_recv.at[d, j], v, chain_to(d))

    groups = CW // 128

    def cut(m, g):
        at = m * CW + g * 128
        return slice(at, at + 128)

    def chain(d, s):
        pos = chip if d else (CHAIN - 1) - chip
        j = s - LAG - pos * HOP

        @pl.when((j >= 0) & (j < CHUNKS))
        def _():
            def local_sum(m):
                return [
                    pb[j, core, d, :, cut(m, g)] + pr[j, d, :, cut(m, g)] for g in range(groups)
                ]

            def wait_received():
                chunk_copy(d, j).wait_recv()
                scale_copy(d, j).wait_recv()

            def with_received(m):
                unit = qr[d, j, :, m * 128 : (m + 1) * 128]
                return [
                    part + rb[d, j, :, cut(m, g)].astype(F32) * unit
                    for g, part in enumerate(local_sum(m))
                ]

            def code(m, parts):
                top = functools.reduce(jnp.maximum, [jnp.abs(p) for p in parts])
                top = jnp.maximum(jnp.max(top, axis=0, keepdims=True), 1e-30)
                up = LEVELS / top
                qs[d, j, :, m * 128 : (m + 1) * 128] = top * (1.0 / LEVELS)
                for g, part in enumerate(parts):
                    sb[d, j, :, cut(m, g)] = (
                        jnp.round(part * up).astype(jnp.int32).astype(jnp.int16)
                    )

            def send():
                scale_copy(d, j).start()
                chunk_copy(d, j).start()

            @pl.when(pos == 0)
            def _():
                for m in range(2):
                    code(m, local_sum(m))
                send()

            @pl.when((pos > 0) & (pos < CHAIN - 1))
            def _():
                wait_received()
                for m in range(2):
                    code(m, with_received(m))
                send()

            @pl.when(pos == CHAIN - 1)
            def _():
                wait_received()
                bits, tok = bt[0], bt[1]
                for m in range(2):
                    logits = with_received(m)
                    high, summed, picked = st[m, 0], st[m, 1], st[m, 2]
                    masked, keeps = [], []
                    for g in range(groups):
                        off = pl.ds(pl.multiple_of(j * CW + g * 128, 128), 128)
                        chosen = colid[:, off] == tok
                        keep = ((bits >> cls[:, off]) & 1 == 1) | chosen
                        picked = picked + jnp.where(chosen, logits[g], 0.0)
                        masked.append(jnp.where(keep, logits[g], NEG))
                        keeps.append(keep)
                    top = functools.reduce(jnp.maximum, masked, high)
                    summed = summed * jnp.exp(high - top)
                    for g in range(groups):
                        summed = summed + jnp.where(keeps[g], jnp.exp(masked[g] - top), 0.0)
                    st[m, 0] = top
                    st[m, 1] = summed
                    st[m, 2] = picked

    def slot(s, carry):
        @pl.when(s < CHUNKS)
        def _():
            multiply(s)
            d2_copy(s).start()

        late = s - LAG

        @pl.when((late >= 0) & (late < CHUNKS))
        def _():
            d2_copy(late).wait_recv()

        chain(1, s)
        chain(0, s)
        return carry

    lax.fori_loop(0, CHUNKS + LAG + (CHAIN - 1) * HOP, slot, 0)

    owner = (chip == 0) | (chip == CHAIN - 1)
    lane1 = lax.broadcasted_iota(jnp.int32, (1, 128), 1)

    def merge(rows):
        total = jnp.sum(rows, axis=0, keepdims=True)
        top = jnp.max(rows, axis=0, keepdims=True)
        lse = top + jnp.log(jnp.sum(jnp.exp(rows - top), axis=0, keepdims=True))
        return jnp.where(lane1 < 64, lse, total)

    def fin_copy(t):
        return remote(
            grow.at[0], gall.at[place], fin_send.at[t], fin_recv.at[place],
            half * PLANE + (place + t) % PLANE, b,
        )

    def z_copy(n):
        hh = (half + n % 2) % 2
        end = chip // 2
        target = end * 3 if n < 2 else 2 - end
        return remote(
            zrow.at[0], zall.at[half], z_send.at[n], z_recv.at[half],
            hh * PLANE + place, target * 2 + core,
        )

    def z_arrived(hh):
        remote(zrow.at[0], zall.at[hh], z_send.at[0], z_recv.at[hh], v, b).wait_recv()

    @pl.when(owner)
    def _():
        total = jnp.zeros((MINE, 128), F32)
        for m in range(2):
            high, summed, picked = (st[m, n] for n in range(3))
            top = jnp.max(high, axis=1, keepdims=True)
            mass = jnp.sum(summed * jnp.exp(high - top), axis=1, keepdims=True)
            lse = jnp.where(mass > 0.0, top + jnp.log(jnp.maximum(mass, 1e-37)), NEG)
            pick = jnp.sum(picked, axis=1, keepdims=True)
            total = total + jnp.where(lane == sub + m * 32, lse, 0.0)
            total = total + jnp.where(lane == sub + m * 32 + 64, pick, 0.0)
        row = jnp.sum(total, axis=0, keepdims=True)
        grow[0] = row
        gall[place] = row

        def start(t, carry):
            fin_copy(t).start()
            return carry

        lax.fori_loop(1, PLANE, start, 0)

        def wait(t, carry):
            n = (place + t) % PLANE
            remote(grow.at[0], gall.at[n], fin_send.at[0], fin_recv.at[n], v, b).wait_recv()
            return carry

        lax.fori_loop(1, PLANE, wait, 0)
        row = merge(gall[...].reshape(PLANE, 128))
        zrow[0] = row
        zall[half] = row
        for n in (3, 1, 2):
            z_copy(n).start()
        z_arrived(1 - half)

    @pl.when(jnp.logical_not(owner))
    def _():
        z_arrived(0)
        z_arrived(1)

    row = merge(zall[...].reshape(2, 128))
    for n in range(4):
        out_ref[n : n + 1, :] = jnp.where(
            chip // 2 == 0, row[:, n * 32 : n * 32 + 16], row[:, n * 32 + 16 : n * 32 + 32]
        )

    pair_copy().wait_send()

    def drain_gather(t, carry):
        sum_copy(t).wait_send()
        near_copy(t).wait_send()
        far_copy(t).wait_send()
        return carry

    lax.fori_loop(1, PLANE, drain_gather, 0)

    def drain_chunks(j, carry):
        d2_copy(j).wait_send()
        return carry

    lax.fori_loop(0, CHUNKS, drain_chunks, 0)
    for d in range(2):
        pos = chip if d else (CHAIN - 1) - chip

        @pl.when(pos < CHAIN - 1)
        def _():
            def drain_chain(j, carry):
                chunk_copy(d, j).wait_send()
                scale_copy(d, j).wait_send()
                return carry

            lax.fori_loop(0, CHUNKS, drain_chain, 0)

    @pl.when(owner)
    def _():
        def drain_final(t, carry):
            fin_copy(t).wait_send()
            return carry

        lax.fori_loop(1, PLANE, drain_final, 0)
        for n in (3, 1, 2):
            z_copy(n).wait_send()


def shards(
    draft_hidden, target_hidden, draft_gain, target_gain, draft_head, target_head,
    token_class, grammar_bits, draft_tokens,
):
    kd, width = draft_head.shape
    kt = target_head.shape[0]
    kk = kd + kt
    vmem, dma = pltpu.VMEM, pltpu.SemaphoreType.DMA
    i32, i16 = jnp.int32, jnp.int16
    scratch = [
        vmem((SHARE, kk), BF16),
        vmem((SHARE, kk), BF16),
        vmem((1, kk), F32),
        vmem((LINE, 1, 128), F32),
        vmem((2 * PLANE, SHARE, kk), BF16),
        vmem((CHUNKS * CW, kd), BF16),
        vmem((CHUNKS * CW, kt), BF16),
        vmem((1, width), i32),
        vmem((1, CHUNKS * CW), i32),
        vmem((1, CHUNKS * CW), i32),
        pltpu.SMEM((ROWS,), i32),
        pltpu.SMEM((ROWS,), i32),
        vmem((4, BLOCK, kk), F32),
        vmem((ROWS, kk), BF16),
        vmem((CHUNKS, 2, 2, MINE, 2 * CW), F32),
        vmem((CHUNKS, 2, MINE, 2 * CW), F32),
        vmem((2, CHUNKS, MINE, 2 * CW), i16),
        vmem((2, CHUNKS, MINE, 2 * CW), i16),
        vmem((2, CHUNKS, 1, 256), F32),
        vmem((2, CHUNKS, 1, 256), F32),
        vmem((2, MINE, 128), i32),
        vmem((2, 3, MINE, 128), F32),
        vmem((1, 1, 128), F32),
        vmem((PLANE, 1, 128), F32),
        vmem((1, 1, 128), F32),
        vmem((2, 1, 128), F32),
        dma((7,)),
        dma((2 * pl.cdiv(width, WSPLIT),)),
        dma((LINE,)),
        dma((LINE,)),
        dma((1,)),
        dma((1,)),
        dma((PLANE,)),
        dma((PLANE,)),
        dma((2 * PLANE,)),
        dma((CHUNKS,)),
        dma((CHUNKS,)),
        dma((2, CHUNKS)),
        dma((2, CHUNKS)),
        dma((2, CHUNKS)),
        dma((2, CHUNKS)),
        dma((PLANE,)),
        dma((PLANE,)),
        dma((4,)),
        dma((2,)),
    ]
    parts = pl.pallas_call(
        functools.partial(kernel, (kd, kt, width)),
        out_shape=jax.ShapeDtypeStruct((4, BLOCK), F32),
        in_specs=[pl.BlockSpec(memory_space=pl.ANY)] * 9,
        out_specs=pl.BlockSpec(memory_space=pltpu.VMEM),
        scratch_shapes=scratch,
        compiler_params=pltpu.CompilerParams(
            collective_id=0, has_side_effects=True, vmem_limit_bytes=62 * 1024 * 1024
        ),
        name="verify",
    )(
        draft_hidden,
        target_hidden,
        draft_gain.reshape(1, kd),
        target_gain.reshape(1, kt),
        draft_head.T,
        target_head.T,
        token_class.reshape(1, width),
        grammar_bits,
        draft_tokens,
    )
    draft_lse, target_lse, draft_pick, target_pick = (parts[n] for n in range(4))
    logprob = target_pick - target_lse
    return logprob - (draft_pick - draft_lse), logprob


def solution(mesh):
    in_specs = (
        P("vocab", "batch"),
        P("vocab", "batch"),
        P("batch"),
        P("batch"),
        P("batch", "vocab"),
        P("batch", "vocab"),
        P("vocab"),
        P(),
        P(),
    )
    out_specs = (P("batch"), P("batch"))
    return jax.shard_map(shards, mesh=mesh, in_specs=in_specs, out_specs=out_specs, check_vma=False)
```

```python
import functools

import jax
import jax.numpy as jnp
from jax import lax
from jax.experimental import pallas as pl
from jax.experimental.pallas import tpu as pltpu
from jax.sharding import PartitionSpec as P

D_DRAFT = 4096
D_TARGET = 8192
EPS = 1e-05
NEG = -1e30
F32 = jnp.float32
BF16 = jnp.bfloat16

PLANE = 16
CHAIN = 4
LINE = 16
ROWS = 128
SHARE = 4
BLOCK = 16
MINE = 32
CW = 256
CHUNKS = 16
LAG = 2
HOP = 4
WSPLIT = 1024
LEVELS = 32760.0


def kernel(
    dims,
    dh, th, dg, tg, wd_hbm, wt_hbm, cls_hbm, bits_hbm, tok_hbm,
    out_ref,
    own, other, gain, sums, xg, wd, wt, cls_in, cls, colid, bits_s, tok_s,
    xf, xn, pb, pr, sb, rb, qs, qr, bt, st,
    grow, gall, zrow, zall,
    load_sem, w_sem, sum_send, sum_recv, pair_send, pair_recv,
    near_send, far_send, g_recv, d2_send, d2_recv,
    c_send, c_recv, q_send, q_recv,
    fin_send, fin_recv, z_send, z_recv,
):
    kd, kt, width = dims
    kk = kd + kt
    v = lax.axis_index("vocab")
    b = lax.axis_index("batch")
    half = v // PLANE
    place = v % PLANE
    chip = b // 2
    core = b % 2
    mate = chip * 2 + (1 - core)
    partner = (v + PLANE) % (2 * PLANE)
    here = half * 8 + b

    def remote(src, dst, send, recv, vv, bb):
        return pltpu.make_async_remote_copy(
            src_ref=src, dst_ref=dst, send_sem=send, recv_sem=recv,
            device_id=(vv, bb), device_id_type=pl.DeviceIdType.MESH,
        )

    barrier = pltpu.get_barrier_semaphore()

    def greet(vv, bb):
        pl.semaphore_signal(
            barrier, inc=1, device_id=(vv, bb), device_id_type=pl.DeviceIdType.MESH
        )

    def greet_line(t, carry):
        to = (here + t) % LINE
        greet((to // 8) * PLANE + place, to % 8)
        return carry

    def greet_plane(t, carry):
        greet(half * PLANE + (place + t) % PLANE, b)
        return carry

    lax.fori_loop(1, LINE, greet_line, 0)
    lax.fori_loop(1, PLANE, greet_plane, 0)

    loads = [
        pltpu.make_async_copy(dh, own.at[:, 0:kd], load_sem.at[0]),
        pltpu.make_async_copy(th, own.at[:, kd:kk], load_sem.at[1]),
        pltpu.make_async_copy(dg, gain.at[:, 0:kd], load_sem.at[2]),
        pltpu.make_async_copy(tg, gain.at[:, kd:kk], load_sem.at[3]),
        pltpu.make_async_copy(cls_hbm, cls_in, load_sem.at[4]),
        pltpu.make_async_copy(bits_hbm, bits_s, load_sem.at[5]),
        pltpu.make_async_copy(tok_hbm, tok_s, load_sem.at[6]),
    ]
    for copy in loads:
        copy.start()
    weights = []
    for hbm, ref in ((wd_hbm, wd), (wt_hbm, wt)):
        for at in range(0, width, WSPLIT):
            rows = pl.ds(at, min(WSPLIT, width - at))
            weights.append((hbm.at[rows], ref.at[rows]))
    weights = [
        pltpu.make_async_copy(src, dst, w_sem.at[n]) for n, (src, dst) in enumerate(weights)
    ]
    for copy in weights:
        copy.start()

    lane4 = lax.broadcasted_iota(jnp.int32, (SHARE, 128), 1)
    sub4 = lax.broadcasted_iota(jnp.int32, (SHARE, 128), 0)
    models = ((0, kd, D_DRAFT), (kd, kk, D_TARGET))
    loads[0].wait()
    loads[1].wait()
    held = jnp.zeros((SHARE, 128), F32)
    for m, (lo, hi, _) in enumerate(models):
        part = own[:, lo:hi].astype(F32)
        square = jnp.sum(part * part, axis=1, keepdims=True)
        held = held + jnp.where(lane4 == sub4 + m * SHARE, square, 0.0)
    sums[here] = jnp.sum(held, axis=0, keepdims=True)

    pl.semaphore_wait(barrier, (LINE - 1) + (PLANE - 1))

    def pair_copy():
        return remote(own, other, pair_send.at[0], pair_recv.at[0], partner, b)

    def sum_copy(t):
        to = (here + t) % LINE
        return remote(
            sums.at[here], sums.at[here], sum_send.at[t], sum_recv.at[here],
            (to // 8) * PLANE + place, to % 8,
        )

    def sum_arrived(n):
        remote(sums.at[n], sums.at[n], sum_send.at[0], sum_recv.at[n], v, b).wait_recv()

    def start_sum(t, carry):
        sum_copy(t).start()
        return carry

    lax.fori_loop(1, LINE, start_sum, 0)
    pair_copy().start()

    for copy in loads[2:]:
        copy.wait()
    lane = lax.broadcasted_iota(jnp.int32, (MINE, 128), 1)
    sub = lax.broadcasted_iota(jnp.int32, (MINE, 128), 0)
    bits_col = jnp.zeros((MINE, 128), jnp.int32)
    tok_col = jnp.zeros((MINE, 128), jnp.int32)
    for stage in range(2):
        at = (stage * 4 + (chip // 2) * 2 + core) * BLOCK
        for r in range(BLOCK):
            row = sub == stage * BLOCK + r
            bits_col = jnp.where(row, bits_s[at + r], bits_col)
            tok_col = jnp.where(row, tok_s[at + r], tok_col)
    bt[0] = bits_col
    bt[1] = tok_col - v * width

    def normalise(rows, n, to):
        total = jnp.sum(sums[pl.ds(n * 8, 8)].reshape(8, 128), axis=0, keepdims=True)
        for m, (lo, hi, depth) in enumerate(models):
            column = jnp.sum(
                jnp.where(lane4 == sub4 + m * SHARE, total, 0.0), axis=1, keepdims=True
            )
            scale = lax.rsqrt(column / depth + EPS)
            xg[to, :, lo:hi] = (rows[:, lo:hi].astype(F32) * scale * gain[:, lo:hi]).astype(BF16)

    def near_copy(t):
        return remote(
            xg.at[v], xg.at[v], near_send.at[t], g_recv.at[v],
            half * PLANE + (place + t) % PLANE, b,
        )

    def far_copy(t):
        return remote(
            xg.at[partner], xg.at[partner], far_send.at[t], g_recv.at[partner],
            half * PLANE + (place + t) % PLANE, b,
        )

    def start_near(t, carry):
        near_copy(t).start()
        return carry

    def start_far(t, carry):
        far_copy(t).start()
        return carry

    def wait_same(t, carry):
        sum_arrived(half * 8 + (b + t) % 8)
        return carry

    def wait_opposite(t, carry):
        sum_arrived((1 - half) * 8 + t)
        return carry

    lax.fori_loop(1, 8, wait_same, 0)
    normalise(own, half, v)
    lax.fori_loop(1, PLANE, start_near, 0)
    lax.fori_loop(0, 8, wait_opposite, 0)
    pair_copy().wait_recv()
    normalise(other, 1 - half, partner)
    lax.fori_loop(1, PLANE, start_far, 0)

    lanes_all = lax.broadcasted_iota(jnp.int32, (1, CHUNKS * CW), 1)
    colid[...] = jnp.where(lanes_all < width, lanes_all, -(1 << 30))
    cls[...] = jnp.full((1, CHUNKS * CW), 30, jnp.int32)
    cls[:, 0:width] = cls_in[...]
    for m in range(2):
        st[m, 0] = jnp.full((MINE, 128), NEG, F32)
        st[m, 1] = jnp.zeros((MINE, 128), F32)
        st[m, 2] = jnp.zeros((MINE, 128), F32)
    for copy in weights:
        copy.wait()
    wd[width:, :] = jnp.zeros((CHUNKS * CW - width, kd), BF16)
    wt[width:, :] = jnp.zeros((CHUNKS * CW - width, kt), BF16)

    def settle(stage, first):
        def wait_row(t, carry):
            n = stage * PLANE + (place + t) % PLANE
            remote(xg.at[n], xg.at[n], near_send.at[0], g_recv.at[n], v, b).wait_recv()
            return carry

        lax.fori_loop(1, PLANE, wait_row, 0)

        def unpack(i, carry):
            for k in range(4):
                xf[i, 4 * k : 4 * k + 4, :] = xg[stage * PLANE + 4 * i + k].astype(F32)
            at = pl.multiple_of((stage * 4 + i) * BLOCK, BLOCK)
            xn[pl.ds(at, BLOCK), :] = xf[i].astype(BF16)
            return carry

        lax.fori_loop(0, 4, unpack, 0)

    settle(half, True)
    settle(1 - half, False)

    def multiply(s):
        for m, ref in enumerate((wd, wt)):
            lo, hi, _ = models[m]
            for n in range(CW // 256):
                at = pl.multiple_of(s * CW + n * 256, 256)
                out = lax.dot_general(
                    xn[:, lo:hi], ref[pl.ds(at, 256), :], (((1,), (1,)), ((), ())),
                    preferred_element_type=F32,
                )
                col = m * CW + n * 256
                for blk in range(ROWS // BLOCK):
                    row = (blk // 4) * BLOCK
                    pb[s, blk % 2, (blk // 2) % 2, row : row + BLOCK, col : col + 256] = out[
                        blk * BLOCK : (blk + 1) * BLOCK
                    ]

    def d2_copy(j):
        return remote(pb.at[j, 1 - core], pr.at[j], d2_send.at[j], d2_recv.at[j], v, mate)

    def chain_to(d):
        return (chip + (1 if d else -1)) * 2 + core

    def chunk_copy(d, j):
        return remote(sb.at[d, j], rb.at[d, j], c_send.at[d, j], c_recv.at[d, j], v, chain_to(d))

    def scale_copy(d, j):
        return remote(qs.at[d, j], qr.at[d, j], q_send.at[d, j], q_recv.at[d, j], v, chain_to(d))

    groups = CW // 128

    def cut(m, g):
        at = m * CW + g * 128
        return slice(at, at + 128)

    def chain(d, s):
        pos = chip if d else (CHAIN - 1) - chip
        j = s - LAG - pos * HOP

        @pl.when((j >= 0) & (j < CHUNKS))
        def _():
            def local_sum(m):
                return [
                    pb[j, core, d, :, cut(m, g)] + pr[j, d, :, cut(m, g)] for g in range(groups)
                ]

            def wait_received():
                chunk_copy(d, j).wait_recv()
                scale_copy(d, j).wait_recv()

            def with_received(m):
                unit = qr[d, j]
                return [
                    part + rb[d, j, :, cut(m, g)].astype(F32) * unit
                    for g, part in enumerate(local_sum(m))
                ]

            def code(parts):
                top = functools.reduce(jnp.maximum, [jnp.abs(p) for p in sum(parts, [])])
                top = jnp.maximum(jnp.max(top, axis=0, keepdims=True), 1e-30)
                up = LEVELS / top
                qs[d, j] = top * (1.0 / LEVELS)
                for m in range(2):
                    for g, part in enumerate(parts[m]):
                        sb[d, j, :, cut(m, g)] = (
                            jnp.round(part * up).astype(jnp.int32).astype(jnp.int16)
                        )

            def send():
                scale_copy(d, j).start()
                chunk_copy(d, j).start()

            @pl.when(pos == 0)
            def _():
                code([local_sum(m) for m in range(2)])
                send()

            @pl.when((pos > 0) & (pos < CHAIN - 1))
            def _():
                wait_received()
                code([with_received(m) for m in range(2)])
                send()

            @pl.when(pos == CHAIN - 1)
            def _():
                wait_received()
                bits, tok = bt[0], bt[1]
                for m in range(2):
                    logits = with_received(m)
                    high, summed, picked = st[m, 0], st[m, 1], st[m, 2]
                    masked, keeps = [], []
                    for g in range(groups):
                        off = pl.ds(pl.multiple_of(j * CW + g * 128, 128), 128)
                        chosen = colid[:, off] == tok
                        keep = ((bits >> cls[:, off]) & 1 == 1) | chosen
                        picked = picked + jnp.where(chosen, logits[g], 0.0)
                        masked.append(jnp.where(keep, logits[g], NEG))
                        keeps.append(keep)
                    top = functools.reduce(jnp.maximum, masked, high)
                    summed = summed * jnp.exp(high - top)
                    for g in range(groups):
                        summed = summed + jnp.where(keeps[g], jnp.exp(masked[g] - top), 0.0)
                    st[m, 0] = top
                    st[m, 1] = summed
                    st[m, 2] = picked

    def slot(s, carry):
        @pl.when(s < CHUNKS)
        def _():
            multiply(s)
            d2_copy(s).start()

        late = s - LAG

        @pl.when((late >= 0) & (late < CHUNKS))
        def _():
            d2_copy(late).wait_recv()

        chain(1, s)
        chain(0, s)
        return carry

    lax.fori_loop(0, CHUNKS + LAG + (CHAIN - 1) * HOP, slot, 0)

    owner = (chip == 0) | (chip == CHAIN - 1)
    lane1 = lax.broadcasted_iota(jnp.int32, (1, 128), 1)

    def merge(rows):
        total = jnp.sum(rows, axis=0, keepdims=True)
        top = jnp.max(rows, axis=0, keepdims=True)
        lse = top + jnp.log(jnp.sum(jnp.exp(rows - top), axis=0, keepdims=True))
        return jnp.where(lane1 < 64, lse, total)

    def fin_copy(t):
        return remote(
            grow.at[0], gall.at[place], fin_send.at[t], fin_recv.at[place],
            half * PLANE + (place + t) % PLANE, b,
        )

    def z_copy(n):
        hh = (half + n % 2) % 2
        end = chip // 2
        target = end * 3 if n < 2 else 2 - end
        return remote(
            zrow.at[0], zall.at[half], z_send.at[n], z_recv.at[half],
            hh * PLANE + place, target * 2 + core,
        )

    def z_arrived(hh):
        remote(zrow.at[0], zall.at[hh], z_send.at[0], z_recv.at[hh], v, b).wait_recv()

    def drain():
        pair_copy().wait_send()

        def drain_gather(t, carry):
            sum_copy(t).wait_send()
            near_copy(t).wait_send()
            far_copy(t).wait_send()
            return carry

        lax.fori_loop(1, PLANE, drain_gather, 0)

        def drain_chunks(j, carry):
            d2_copy(j).wait_send()
            return carry

        lax.fori_loop(0, CHUNKS, drain_chunks, 0)
        for d in range(2):
            pos = chip if d else (CHAIN - 1) - chip

            @pl.when(pos < CHAIN - 1)
            def _():
                def drain_chain(j, carry):
                    chunk_copy(d, j).wait_send()
                    scale_copy(d, j).wait_send()
                    return carry

                lax.fori_loop(0, CHUNKS, drain_chain, 0)

    @pl.when(owner)
    def _():
        total = jnp.zeros((MINE, 128), F32)
        for m in range(2):
            high, summed, picked = (st[m, n] for n in range(3))
            top = jnp.max(high, axis=1, keepdims=True)
            mass = jnp.sum(summed * jnp.exp(high - top), axis=1, keepdims=True)
            lse = jnp.where(mass > 0.0, top + jnp.log(jnp.maximum(mass, 1e-37)), NEG)
            pick = jnp.sum(picked, axis=1, keepdims=True)
            total = total + jnp.where(lane == sub + m * 32, lse, 0.0)
            total = total + jnp.where(lane == sub + m * 32 + 64, pick, 0.0)
        row = jnp.sum(total, axis=0, keepdims=True)
        grow[0] = row
        gall[place] = row

        def start(t, carry):
            fin_copy(t).start()
            return carry

        lax.fori_loop(1, PLANE, start, 0)
        drain()

        def wait(t, carry):
            n = (place + t) % PLANE
            remote(grow.at[0], gall.at[n], fin_send.at[0], fin_recv.at[n], v, b).wait_recv()
            return carry

        lax.fori_loop(1, PLANE, wait, 0)
        row = merge(gall[...].reshape(PLANE, 128))
        zrow[0] = row
        zall[half] = row
        for n in (3, 1, 2):
            z_copy(n).start()

        def drain_final(t, carry):
            fin_copy(t).wait_send()
            return carry

        lax.fori_loop(1, PLANE, drain_final, 0)
        for n in (3, 1, 2):
            z_copy(n).wait_send()
        z_arrived(1 - half)

    @pl.when(jnp.logical_not(owner))
    def _():
        drain()
        z_arrived(0)
        z_arrived(1)

    row = merge(zall[...].reshape(2, 128))
    for n in range(4):
        out_ref[n : n + 1, :] = jnp.where(
            chip // 2 == 0, row[:, n * 32 : n * 32 + 16], row[:, n * 32 + 16 : n * 32 + 32]
        )


def shards(
    draft_hidden, target_hidden, draft_gain, target_gain, draft_head, target_head,
    token_class, grammar_bits, draft_tokens,
):
    kd, width = draft_head.shape
    kt = target_head.shape[0]
    kk = kd + kt
    vmem, dma = pltpu.VMEM, pltpu.SemaphoreType.DMA
    i32, i16 = jnp.int32, jnp.int16
    scratch = [
        vmem((SHARE, kk), BF16),
        vmem((SHARE, kk), BF16),
        vmem((1, kk), F32),
        vmem((LINE, 1, 128), F32),
        vmem((2 * PLANE, SHARE, kk), BF16),
        vmem((CHUNKS * CW, kd), BF16),
        vmem((CHUNKS * CW, kt), BF16),
        vmem((1, width), i32),
        vmem((1, CHUNKS * CW), i32),
        vmem((1, CHUNKS * CW), i32),
        pltpu.SMEM((ROWS,), i32),
        pltpu.SMEM((ROWS,), i32),
        vmem((4, BLOCK, kk), F32),
        vmem((ROWS, kk), BF16),
        vmem((CHUNKS, 2, 2, MINE, 2 * CW), F32),
        vmem((CHUNKS, 2, MINE, 2 * CW), F32),
        vmem((2, CHUNKS, MINE, 2 * CW), i16),
        vmem((2, CHUNKS, MINE, 2 * CW), i16),
        vmem((2, CHUNKS, 1, 128), F32),
        vmem((2, CHUNKS, 1, 128), F32),
        vmem((2, MINE, 128), i32),
        vmem((2, 3, MINE, 128), F32),
        vmem((1, 1, 128), F32),
        vmem((PLANE, 1, 128), F32),
        vmem((1, 1, 128), F32),
        vmem((2, 1, 128), F32),
        dma((7,)),
        dma((2 * pl.cdiv(width, WSPLIT),)),
        dma((LINE,)),
        dma((LINE,)),
        dma((1,)),
        dma((1,)),
        dma((PLANE,)),
        dma((PLANE,)),
        dma((2 * PLANE,)),
        dma((CHUNKS,)),
        dma((CHUNKS,)),
        dma((2, CHUNKS)),
        dma((2, CHUNKS)),
        dma((2, CHUNKS)),
        dma((2, CHUNKS)),
        dma((PLANE,)),
        dma((PLANE,)),
        dma((4,)),
        dma((2,)),
    ]
    parts = pl.pallas_call(
        functools.partial(kernel, (kd, kt, width)),
        out_shape=pltpu.VMEM((4, BLOCK), F32),
        in_specs=[pl.BlockSpec(memory_space=pl.ANY)] * 9,
        out_specs=pl.BlockSpec(memory_space=pltpu.VMEM),
        scratch_shapes=scratch,
        compiler_params=pltpu.CompilerParams(
            collective_id=0, has_side_effects=True, vmem_limit_bytes=62 * 1024 * 1024
        ),
        name="verify",
    )(
        draft_hidden,
        target_hidden,
        draft_gain.reshape(1, kd),
        target_gain.reshape(1, kt),
        draft_head.T,
        target_head.T,
        token_class.reshape(1, width),
        grammar_bits,
        draft_tokens,
    )
    draft_lse, target_lse, draft_pick, target_pick = (parts[n] for n in range(4))
    logprob = target_pick - target_lse
    return logprob - (draft_pick - draft_lse), logprob


def solution(mesh):
    in_specs = (
        P("vocab", "batch"),
        P("vocab", "batch"),
        P("batch"),
        P("batch"),
        P("batch", "vocab"),
        P("batch", "vocab"),
        P("vocab"),
        P(),
        P(),
    )
    out_specs = (P("batch"), P("batch"))
    return jax.shard_map(shards, mesh=mesh, in_specs=in_specs, out_specs=out_specs, check_vma=False)
```

```python
import functools

import jax
import jax.numpy as jnp
from jax import lax
from jax.experimental import pallas as pl
from jax.experimental.pallas import tpu as pltpu
from jax.sharding import PartitionSpec as P

D_DRAFT = 4096
D_TARGET = 8192
EPS = 1e-05
NEG = -1e30
F32 = jnp.float32
BF16 = jnp.bfloat16

PLANE = 16
AWAY = (10, 6, 9, 11, 14, 5, 7, 13, 2, 8, 15, 3, 1, 4, 12)
CHAIN = 4
LINE = 16
ROWS = 128
SHARE = 4
BLOCK = 16
MINE = 32
CW = 256
CHUNKS = 16
LAG = 2
HOP = 4
WSPLIT = 1024
LEVELS = 32760.0


def kernel(
    dims,
    dh, th, dg, tg, wd_hbm, wt_hbm, cls_hbm, bits_hbm, tok_hbm,
    out_ref,
    own, other, gain, sums, xg, wd, wt, cls_in, cls, colid, bits_s, tok_s,
    xf, xn, pb, pr, sb, rb, qs, qr, bt, st,
    grow, gall, zrow, zall,
    load_sem, w_sem, sum_send, sum_recv, pair_send, pair_recv,
    near_send, far_send, g_recv, d2_send, d2_recv,
    c_send, c_recv, q_send, q_recv,
    fin_send, fin_recv, z_send, z_recv,
):
    kd, kt, width = dims
    kk = kd + kt
    v = lax.axis_index("vocab")
    b = lax.axis_index("batch")
    half = v // PLANE
    place = v % PLANE
    chip = b // 2
    core = b % 2
    mate = chip * 2 + (1 - core)
    partner = (v + PLANE) % (2 * PLANE)
    here = half * 8 + b

    def remote(src, dst, send, recv, vv, bb):
        return pltpu.make_async_remote_copy(
            src_ref=src, dst_ref=dst, send_sem=send, recv_sem=recv,
            device_id=(vv, bb), device_id_type=pl.DeviceIdType.MESH,
        )

    barrier = pltpu.get_barrier_semaphore()

    def greet(vv, bb):
        pl.semaphore_signal(
            barrier, inc=1, device_id=(vv, bb), device_id_type=pl.DeviceIdType.MESH
        )

    for t in AWAY:
        greet(half * PLANE + (place + t) % PLANE, b)
        to = (here + t) % LINE
        greet((to // 8) * PLANE + place, to % 8)

    loads = [
        pltpu.make_async_copy(dh, own.at[:, 0:kd], load_sem.at[0]),
        pltpu.make_async_copy(th, own.at[:, kd:kk], load_sem.at[1]),
        pltpu.make_async_copy(dg, gain.at[:, 0:kd], load_sem.at[2]),
        pltpu.make_async_copy(tg, gain.at[:, kd:kk], load_sem.at[3]),
        pltpu.make_async_copy(cls_hbm, cls_in, load_sem.at[4]),
        pltpu.make_async_copy(bits_hbm, bits_s, load_sem.at[5]),
        pltpu.make_async_copy(tok_hbm, tok_s, load_sem.at[6]),
    ]
    for copy in loads:
        copy.start()
    weights = []
    for hbm, ref in ((wd_hbm, wd), (wt_hbm, wt)):
        for at in range(0, width, WSPLIT):
            rows = pl.ds(at, min(WSPLIT, width - at))
            weights.append((hbm.at[rows], ref.at[rows]))
    weights = [
        pltpu.make_async_copy(src, dst, w_sem.at[n]) for n, (src, dst) in enumerate(weights)
    ]
    for copy in weights:
        copy.start()

    lane4 = lax.broadcasted_iota(jnp.int32, (SHARE, 128), 1)
    sub4 = lax.broadcasted_iota(jnp.int32, (SHARE, 128), 0)
    models = ((0, kd, D_DRAFT), (kd, kk, D_TARGET))
    loads[0].wait()
    loads[1].wait()
    held = jnp.zeros((SHARE, 128), F32)
    for m, (lo, hi, _) in enumerate(models):
        part = own[:, lo:hi].astype(F32)
        square = jnp.sum(part * part, axis=1, keepdims=True)
        held = held + jnp.where(lane4 == sub4 + m * SHARE, square, 0.0)
    sums[here] = jnp.sum(held, axis=0, keepdims=True)

    pl.semaphore_wait(barrier, (LINE - 1) + (PLANE - 1))

    def pair_copy():
        return remote(own, other, pair_send.at[0], pair_recv.at[0], partner, b)

    def sum_copy(t):
        to = (here + t) % LINE
        return remote(
            sums.at[here], sums.at[here], sum_send.at[t], sum_recv.at[here],
            (to // 8) * PLANE + place, to % 8,
        )

    def sum_arrived(n):
        remote(sums.at[n], sums.at[n], sum_send.at[0], sum_recv.at[n], v, b).wait_recv()

    def start_sum(t, carry):
        sum_copy(t).start()
        return carry

    pair_copy().start()
    for t in (8, 9, 7, 10, 6, 11, 5, 12, 4, 13, 3, 14, 2, 15, 1):
        sum_copy(t).start()

    for copy in loads[2:]:
        copy.wait()
    lane = lax.broadcasted_iota(jnp.int32, (MINE, 128), 1)
    sub = lax.broadcasted_iota(jnp.int32, (MINE, 128), 0)
    bits_col = jnp.zeros((MINE, 128), jnp.int32)
    tok_col = jnp.zeros((MINE, 128), jnp.int32)
    for stage in range(2):
        at = ((1 - chip // 2) * 4 + stage * 2 + core) * BLOCK
        for r in range(BLOCK):
            row = sub == stage * BLOCK + r
            bits_col = jnp.where(row, bits_s[at + r], bits_col)
            tok_col = jnp.where(row, tok_s[at + r], tok_col)
    bt[0] = bits_col
    bt[1] = tok_col - v * width

    def normalise(rows, n, to):
        total = jnp.sum(sums[pl.ds(n * 8, 8)].reshape(8, 128), axis=0, keepdims=True)
        for m, (lo, hi, depth) in enumerate(models):
            column = jnp.sum(
                jnp.where(lane4 == sub4 + m * SHARE, total, 0.0), axis=1, keepdims=True
            )
            scale = lax.rsqrt(column / depth + EPS)
            xg[to, :, lo:hi] = (rows[:, lo:hi].astype(F32) * scale * gain[:, lo:hi]).astype(BF16)

    def near_copy(t):
        return remote(
            xg.at[v], xg.at[v], near_send.at[t], g_recv.at[v],
            half * PLANE + (place + t) % PLANE, b,
        )

    def far_copy(t):
        return remote(
            xg.at[partner], xg.at[partner], far_send.at[t], g_recv.at[partner],
            half * PLANE + (place + t) % PLANE, b,
        )

    def start_near(t, carry):
        near_copy(t).start()
        return carry

    def start_far(t, carry):
        far_copy(t).start()
        return carry

    def wait_same(t, carry):
        sum_arrived(half * 8 + (b + t) % 8)
        return carry

    def wait_opposite(t, carry):
        sum_arrived((1 - half) * 8 + t)
        return carry

    lax.fori_loop(1, 8, wait_same, 0)
    normalise(own, half, v)
    for t in AWAY:
        near_copy(t).start()
    lax.fori_loop(0, 8, wait_opposite, 0)
    pair_copy().wait_recv()
    normalise(other, 1 - half, partner)
    for t in AWAY:
        far_copy(t).start()

    lanes_all = lax.broadcasted_iota(jnp.int32, (1, CHUNKS * CW), 1)
    colid[...] = jnp.where(lanes_all < width, lanes_all, -(1 << 30))
    cls[...] = jnp.full((1, CHUNKS * CW), 30, jnp.int32)
    cls[:, 0:width] = cls_in[...]
    for m in range(2):
        st[m, 0] = jnp.full((MINE, 128), NEG, F32)
        st[m, 1] = jnp.zeros((MINE, 128), F32)
        st[m, 2] = jnp.zeros((MINE, 128), F32)
    for copy in weights:
        copy.wait()
    wd[width:, :] = jnp.zeros((CHUNKS * CW - width, kd), BF16)
    wt[width:, :] = jnp.zeros((CHUNKS * CW - width, kt), BF16)

    def settle(stage, first):
        def wait_row(t, carry):
            n = stage * PLANE + (place + t) % PLANE
            remote(xg.at[n], xg.at[n], near_send.at[0], g_recv.at[n], v, b).wait_recv()
            return carry

        lax.fori_loop(1, PLANE, wait_row, 0)

        def unpack(i, carry):
            for k in range(4):
                xf[i, 4 * k : 4 * k + 4, :] = xg[stage * PLANE + 4 * i + k].astype(F32)
            at = pl.multiple_of((stage * 4 + i) * BLOCK, BLOCK)
            xn[pl.ds(at, BLOCK), :] = xf[i].astype(BF16)
            return carry

        lax.fori_loop(0, 4, unpack, 0)

    settle(half, True)
    settle(1 - half, False)

    def multiply(s):
        for m, ref in enumerate((wd, wt)):
            lo, hi, _ = models[m]
            for n in range(CW // 256):
                at = pl.multiple_of(s * CW + n * 256, 256)
                out = lax.dot_general(
                    xn[:, lo:hi], ref[pl.ds(at, 256), :], (((1,), (1,)), ((), ())),
                    preferred_element_type=F32,
                )
                col = m * CW + n * 256
                for blk in range(ROWS // BLOCK):
                    row = (blk // 2) % 2 * BLOCK
                    pb[s, blk % 2, 1 - blk // 4, row : row + BLOCK, col : col + 256] = out[
                        blk * BLOCK : (blk + 1) * BLOCK
                    ]

    def d2_copy(j):
        return remote(pb.at[j, 1 - core], pr.at[j], d2_send.at[j], d2_recv.at[j], v, mate)

    def chain_to(d):
        return (chip + (1 if d else -1)) * 2 + core

    def chunk_copy(d, j):
        return remote(sb.at[d, j], rb.at[d, j], c_send.at[d, j], c_recv.at[d, j], v, chain_to(d))

    def scale_copy(d, j):
        return remote(qs.at[d, j], qr.at[d, j], q_send.at[d, j], q_recv.at[d, j], v, chain_to(d))

    groups = CW // 128

    def cut(m, g):
        at = m * CW + g * 128
        return slice(at, at + 128)

    def chain(d, s):
        pos = chip if d else (CHAIN - 1) - chip
        j = s - LAG - pos * HOP

        @pl.when((j >= 0) & (j < CHUNKS))
        def _():
            def local_sum(m):
                return [
                    pb[j, core, d, :, cut(m, g)] + pr[j, d, :, cut(m, g)] for g in range(groups)
                ]

            def wait_received():
                chunk_copy(d, j).wait_recv()
                scale_copy(d, j).wait_recv()

            def with_received(m):
                unit = qr[d, j]
                return [
                    part + rb[d, j, :, cut(m, g)].astype(F32) * unit
                    for g, part in enumerate(local_sum(m))
                ]

            def code(parts):
                top = functools.reduce(jnp.maximum, [jnp.abs(p) for p in sum(parts, [])])
                top = jnp.maximum(jnp.max(top, axis=0, keepdims=True), 1e-30)
                up = LEVELS / top
                qs[d, j] = top * (1.0 / LEVELS)
                for m in range(2):
                    for g, part in enumerate(parts[m]):
                        sb[d, j, :, cut(m, g)] = (
                            jnp.round(part * up).astype(jnp.int32).astype(jnp.int16)
                        )

            def send():
                scale_copy(d, j).start()
                chunk_copy(d, j).start()

            @pl.when(pos == 0)
            def _():
                code([local_sum(m) for m in range(2)])
                send()

            @pl.when((pos > 0) & (pos < CHAIN - 1))
            def _():
                wait_received()
                code([with_received(m) for m in range(2)])
                send()

            @pl.when(pos == CHAIN - 1)
            def _():
                wait_received()
                bits, tok = bt[0], bt[1]
                for m in range(2):
                    logits = with_received(m)
                    high, summed, picked = st[m, 0], st[m, 1], st[m, 2]
                    masked, keeps = [], []
                    for g in range(groups):
                        off = pl.ds(pl.multiple_of(j * CW + g * 128, 128), 128)
                        chosen = colid[:, off] == tok
                        keep = ((bits >> cls[:, off]) & 1 == 1) | chosen
                        picked = picked + jnp.where(chosen, logits[g], 0.0)
                        masked.append(jnp.where(keep, logits[g], NEG))
                        keeps.append(keep)
                    top = functools.reduce(jnp.maximum, masked, high)
                    summed = summed * jnp.exp(high - top)
                    for g in range(groups):
                        summed = summed + jnp.where(keeps[g], jnp.exp(masked[g] - top), 0.0)
                    st[m, 0] = top
                    st[m, 1] = summed
                    st[m, 2] = picked

    def slot(s, carry):
        @pl.when(s < CHUNKS)
        def _():
            multiply(s)
            d2_copy(s).start()

        late = s - LAG

        @pl.when((late >= 0) & (late < CHUNKS))
        def _():
            d2_copy(late).wait_recv()

        chain(1, s)
        chain(0, s)
        return carry

    lax.fori_loop(0, CHUNKS + LAG + (CHAIN - 1) * HOP, slot, 0)

    owner = (chip == 0) | (chip == CHAIN - 1)
    lane1 = lax.broadcasted_iota(jnp.int32, (1, 128), 1)

    def merge(rows):
        total = jnp.sum(rows, axis=0, keepdims=True)
        top = jnp.max(rows, axis=0, keepdims=True)
        lse = top + jnp.log(jnp.sum(jnp.exp(rows - top), axis=0, keepdims=True))
        return jnp.where(lane1 < 64, lse, total)

    def fin_copy(t):
        return remote(
            grow.at[0], gall.at[place], fin_send.at[t], fin_recv.at[place],
            half * PLANE + (place + t) % PLANE, b,
        )

    def z_copy(n):
        hh = (half + n % 2) % 2
        target = (1 - chip // 2) * 2 + n // 2
        return remote(
            zrow.at[0], zall.at[half], z_send.at[n], z_recv.at[half],
            hh * PLANE + place, target * 2 + core,
        )

    def z_arrived(hh):
        remote(zrow.at[0], zall.at[hh], z_send.at[0], z_recv.at[hh], v, b).wait_recv()

    def drain():
        pair_copy().wait_send()

        def drain_gather(t, carry):
            sum_copy(t).wait_send()
            near_copy(t).wait_send()
            far_copy(t).wait_send()
            return carry

        lax.fori_loop(1, PLANE, drain_gather, 0)

        def drain_chunks(j, carry):
            d2_copy(j).wait_send()
            return carry

        lax.fori_loop(0, CHUNKS, drain_chunks, 0)
        for d in range(2):
            pos = chip if d else (CHAIN - 1) - chip

            @pl.when(pos < CHAIN - 1)
            def _():
                def drain_chain(j, carry):
                    chunk_copy(d, j).wait_send()
                    scale_copy(d, j).wait_send()
                    return carry

                lax.fori_loop(0, CHUNKS, drain_chain, 0)

    @pl.when(owner)
    def _():
        total = jnp.zeros((MINE, 128), F32)
        for m in range(2):
            high, summed, picked = (st[m, n] for n in range(3))
            top = jnp.max(high, axis=1, keepdims=True)
            mass = jnp.sum(summed * jnp.exp(high - top), axis=1, keepdims=True)
            lse = jnp.where(mass > 0.0, top + jnp.log(jnp.maximum(mass, 1e-37)), NEG)
            pick = jnp.sum(picked, axis=1, keepdims=True)
            total = total + jnp.where(lane == sub + m * 32, lse, 0.0)
            total = total + jnp.where(lane == sub + m * 32 + 64, pick, 0.0)
        row = jnp.sum(total, axis=0, keepdims=True)
        grow[0] = row
        gall[place] = row

        for t in AWAY:
            fin_copy(t).start()
        drain()

        def wait(t, carry):
            n = (place + t) % PLANE
            remote(grow.at[0], gall.at[n], fin_send.at[0], fin_recv.at[n], v, b).wait_recv()
            return carry

        lax.fori_loop(1, PLANE, wait, 0)
        row = merge(gall[...].reshape(PLANE, 128))
        zrow[0] = row
        for n in range(4):
            z_copy(n).start()

        def drain_final(t, carry):
            fin_copy(t).wait_send()
            return carry

        lax.fori_loop(1, PLANE, drain_final, 0)
        for n in range(4):
            z_copy(n).wait_send()

    @pl.when(jnp.logical_not(owner))
    def _():
        drain()

    z_arrived(0)
    z_arrived(1)
    row = merge(zall[...].reshape(2, 128))
    for n in range(4):
        out_ref[n : n + 1, :] = jnp.where(
            chip % 2 == 0, row[:, n * 32 : n * 32 + 16], row[:, n * 32 + 16 : n * 32 + 32]
        )


def shards(
    draft_hidden, target_hidden, draft_gain, target_gain, draft_head, target_head,
    token_class, grammar_bits, draft_tokens,
):
    kd, width = draft_head.shape
    kt = target_head.shape[0]
    kk = kd + kt
    vmem, dma = pltpu.VMEM, pltpu.SemaphoreType.DMA
    i32, i16 = jnp.int32, jnp.int16
    scratch = [
        vmem((SHARE, kk), BF16),
        vmem((SHARE, kk), BF16),
        vmem((1, kk), F32),
        vmem((LINE, 1, 128), F32),
        vmem((2 * PLANE, SHARE, kk), BF16),
        vmem((CHUNKS * CW, kd), BF16),
        vmem((CHUNKS * CW, kt), BF16),
        vmem((1, width), i32),
        vmem((1, CHUNKS * CW), i32),
        vmem((1, CHUNKS * CW), i32),
        pltpu.SMEM((ROWS,), i32),
        pltpu.SMEM((ROWS,), i32),
        vmem((4, BLOCK, kk), F32),
        vmem((ROWS, kk), BF16),
        vmem((CHUNKS, 2, 2, MINE, 2 * CW), F32),
        vmem((CHUNKS, 2, MINE, 2 * CW), F32),
        vmem((2, CHUNKS, MINE, 2 * CW), i16),
        vmem((2, CHUNKS, MINE, 2 * CW), i16),
        vmem((2, CHUNKS, 1, 128), F32),
        vmem((2, CHUNKS, 1, 128), F32),
        vmem((2, MINE, 128), i32),
        vmem((2, 3, MINE, 128), F32),
        vmem((1, 1, 128), F32),
        vmem((PLANE, 1, 128), F32),
        vmem((1, 1, 128), F32),
        vmem((2, 1, 128), F32),
        dma((7,)),
        dma((2 * pl.cdiv(width, WSPLIT),)),
        dma((LINE,)),
        dma((LINE,)),
        dma((1,)),
        dma((1,)),
        dma((PLANE,)),
        dma((PLANE,)),
        dma((2 * PLANE,)),
        dma((CHUNKS,)),
        dma((CHUNKS,)),
        dma((2, CHUNKS)),
        dma((2, CHUNKS)),
        dma((2, CHUNKS)),
        dma((2, CHUNKS)),
        dma((PLANE,)),
        dma((PLANE,)),
        dma((4,)),
        dma((2,)),
    ]
    parts = pl.pallas_call(
        functools.partial(kernel, (kd, kt, width)),
        out_shape=pltpu.VMEM((4, BLOCK), F32),
        in_specs=[pl.BlockSpec(memory_space=pl.ANY)] * 9,
        out_specs=pl.BlockSpec(memory_space=pltpu.VMEM),
        scratch_shapes=scratch,
        compiler_params=pltpu.CompilerParams(
            collective_id=0, has_side_effects=True, vmem_limit_bytes=62 * 1024 * 1024
        ),
        name="verify",
    )(
        draft_hidden,
        target_hidden,
        draft_gain.reshape(1, kd),
        target_gain.reshape(1, kt),
        draft_head.T,
        target_head.T,
        token_class.reshape(1, width),
        grammar_bits,
        draft_tokens,
    )
    draft_lse, target_lse, draft_pick, target_pick = (parts[n] for n in range(4))
    logprob = target_pick - target_lse
    return logprob - (draft_pick - draft_lse), logprob


def solution(mesh):
    in_specs = (
        P("vocab", "batch"),
        P("vocab", "batch"),
        P("batch"),
        P("batch"),
        P("batch", "vocab"),
        P("batch", "vocab"),
        P("vocab"),
        P(),
        P(),
    )
    out_specs = (P("batch"), P("batch"))
    return jax.shard_map(shards, mesh=mesh, in_specs=in_specs, out_specs=out_specs, check_vma=False)
```

```python
import functools

import jax
import jax.numpy as jnp
from jax import lax
from jax.experimental import pallas as pl
from jax.experimental.pallas import tpu as pltpu
from jax.sharding import PartitionSpec as P

D_DRAFT = 4096
D_TARGET = 8192
EPS = 1e-05
NEG = -1e30
F32 = jnp.float32
BF16 = jnp.bfloat16

PLANE = 16
AWAY = (10, 6, 9, 11, 14, 5, 7, 13, 2, 8, 15, 3, 1, 4, 12)
CHAIN = 4
LINE = 16
ROWS = 128
SHARE = 4
BLOCK = 16
MINE = 32
CW = 256
CHUNKS = 16
LAG = 2
HOP = 4
WSPLIT = 1024
LEVELS = 32760.0


def kernel(
    dims,
    dh, th, dg, tg, wd_hbm, wt_hbm, cls_hbm, bits_hbm, tok_hbm,
    out_ref,
    own, other, gain, sums, xg, wd, wt, cls_in, cls, colid, bits_s, tok_s,
    xf, xn, pb, pr, sb, rb, qs, qr, bt, st,
    grow, gall, zrow, zall,
    load_sem, w_sem, sum_send, sum_recv, pair_send, pair_recv,
    near_send, far_send, g_recv, d2_send, d2_recv,
    c_send, c_recv, q_send, q_recv,
    fin_send, fin_recv, z_send, z_recv,
):
    kd, kt, width = dims
    kk = kd + kt
    v = lax.axis_index("vocab")
    b = lax.axis_index("batch")
    half = v // PLANE
    place = v % PLANE
    chip = b // 2
    core = b % 2
    mate = chip * 2 + (1 - core)
    partner = (v + PLANE) % (2 * PLANE)
    here = half * 8 + b

    def remote(src, dst, send, recv, vv, bb):
        return pltpu.make_async_remote_copy(
            src_ref=src, dst_ref=dst, send_sem=send, recv_sem=recv,
            device_id=(vv, bb), device_id_type=pl.DeviceIdType.MESH,
        )

    barrier = pltpu.get_barrier_semaphore()

    def greet(vv, bb):
        pl.semaphore_signal(
            barrier, inc=1, device_id=(vv, bb), device_id_type=pl.DeviceIdType.MESH
        )

    for t in AWAY:
        greet(half * PLANE + (place + t) % PLANE, b)
        to = (here + t) % LINE
        greet((to // 8) * PLANE + place, to % 8)

    loads = [
        pltpu.make_async_copy(dh, own.at[:, 0:kd], load_sem.at[0]),
        pltpu.make_async_copy(th, own.at[:, kd:kk], load_sem.at[1]),
        pltpu.make_async_copy(dg, gain.at[:, 0:kd], load_sem.at[2]),
        pltpu.make_async_copy(tg, gain.at[:, kd:kk], load_sem.at[3]),
        pltpu.make_async_copy(cls_hbm, cls_in, load_sem.at[4]),
        pltpu.make_async_copy(bits_hbm, bits_s, load_sem.at[5]),
        pltpu.make_async_copy(tok_hbm, tok_s, load_sem.at[6]),
    ]
    for copy in loads:
        copy.start()
    weights = []
    for hbm, ref in ((wd_hbm, wd), (wt_hbm, wt)):
        for at in range(0, width, WSPLIT):
            rows = pl.ds(at, min(WSPLIT, width - at))
            weights.append((hbm.at[rows], ref.at[rows]))
    weights = [
        pltpu.make_async_copy(src, dst, w_sem.at[n]) for n, (src, dst) in enumerate(weights)
    ]
    for copy in weights:
        copy.start()

    lane4 = lax.broadcasted_iota(jnp.int32, (SHARE, 128), 1)
    sub4 = lax.broadcasted_iota(jnp.int32, (SHARE, 128), 0)
    models = ((0, kd, D_DRAFT), (kd, kk, D_TARGET))
    loads[0].wait()
    loads[1].wait()
    held = jnp.zeros((SHARE, 128), F32)
    for m, (lo, hi, _) in enumerate(models):
        part = own[:, lo:hi].astype(F32)
        square = jnp.sum(part * part, axis=1, keepdims=True)
        held = held + jnp.where(lane4 == sub4 + m * SHARE, square, 0.0)
    sums[here] = jnp.sum(held, axis=0, keepdims=True)

    pl.semaphore_wait(barrier, (LINE - 1) + (PLANE - 1))

    def pair_copy():
        return remote(own, other, pair_send.at[0], pair_recv.at[0], partner, b)

    def sum_copy(t):
        to = (here + t) % LINE
        return remote(
            sums.at[here], sums.at[here], sum_send.at[t], sum_recv.at[here],
            (to // 8) * PLANE + place, to % 8,
        )

    def sum_arrived(n):
        remote(sums.at[n], sums.at[n], sum_send.at[0], sum_recv.at[n], v, b).wait_recv()

    def start_sum(t, carry):
        sum_copy(t).start()
        return carry

    pair_copy().start()
    for t in (8, 9, 7, 10, 6, 11, 5, 12, 4, 13, 3, 14, 2, 15, 1):
        sum_copy(t).start()

    for copy in loads[2:]:
        copy.wait()
    lane = lax.broadcasted_iota(jnp.int32, (MINE, 128), 1)
    sub = lax.broadcasted_iota(jnp.int32, (MINE, 128), 0)
    bits_col = jnp.zeros((MINE, 128), jnp.int32)
    tok_col = jnp.zeros((MINE, 128), jnp.int32)
    for stage in range(2):
        at = ((1 - chip // 2) * 4 + stage * 2 + core) * BLOCK
        for r in range(BLOCK):
            row = sub == stage * BLOCK + r
            bits_col = jnp.where(row, bits_s[at + r], bits_col)
            tok_col = jnp.where(row, tok_s[at + r], tok_col)
    bt[0] = bits_col
    bt[1] = tok_col - v * width

    def normalise(rows, n, to):
        total = jnp.sum(sums[pl.ds(n * 8, 8)].reshape(8, 128), axis=0, keepdims=True)
        for m, (lo, hi, depth) in enumerate(models):
            column = jnp.sum(
                jnp.where(lane4 == sub4 + m * SHARE, total, 0.0), axis=1, keepdims=True
            )
            scale = lax.rsqrt(column / depth + EPS)
            xg[to, :, lo:hi] = (rows[:, lo:hi].astype(F32) * scale * gain[:, lo:hi]).astype(BF16)

    def near_copy(t):
        return remote(
            xg.at[v], xg.at[v], near_send.at[t], g_recv.at[v],
            half * PLANE + (place + t) % PLANE, b,
        )

    def far_copy(t):
        return remote(
            xg.at[partner], xg.at[partner], far_send.at[t], g_recv.at[partner],
            half * PLANE + (place + t) % PLANE, b,
        )

    def start_near(t, carry):
        near_copy(t).start()
        return carry

    def start_far(t, carry):
        far_copy(t).start()
        return carry

    def wait_same(t, carry):
        sum_arrived(half * 8 + (b + t) % 8)
        return carry

    def wait_opposite(t, carry):
        sum_arrived((1 - half) * 8 + t)
        return carry

    lax.fori_loop(1, 8, wait_same, 0)
    normalise(own, half, v)
    for t in AWAY:
        near_copy(t).start()
    lax.fori_loop(0, 8, wait_opposite, 0)
    pair_copy().wait_recv()
    normalise(other, 1 - half, partner)
    for t in AWAY:
        far_copy(t).start()

    lanes_all = lax.broadcasted_iota(jnp.int32, (1, CHUNKS * CW), 1)
    colid[...] = jnp.where(lanes_all < width, lanes_all, -(1 << 30))
    cls[...] = jnp.full((1, CHUNKS * CW), 30, jnp.int32)
    cls[:, 0:width] = cls_in[...]
    for m in range(2):
        st[m, 0] = jnp.full((MINE, 128), NEG, F32)
        st[m, 1] = jnp.zeros((MINE, 128), F32)
        st[m, 2] = jnp.zeros((MINE, 128), F32)
    for copy in weights:
        copy.wait()
    wd[width:, :] = jnp.zeros((CHUNKS * CW - width, kd), BF16)
    wt[width:, :] = jnp.zeros((CHUNKS * CW - width, kt), BF16)

    def settle(stage, first):
        def wait_row(t, carry):
            n = stage * PLANE + (place + t) % PLANE
            remote(xg.at[n], xg.at[n], near_send.at[0], g_recv.at[n], v, b).wait_recv()
            return carry

        lax.fori_loop(1, PLANE, wait_row, 0)

        def unpack(i, carry):
            for k in range(4):
                xf[i, 4 * k : 4 * k + 4, :] = xg[stage * PLANE + 4 * i + k].astype(F32)
            at = pl.multiple_of((stage * 4 + i) * BLOCK, BLOCK)
            xn[pl.ds(at, BLOCK), :] = xf[i].astype(BF16)
            return carry

        lax.fori_loop(0, 4, unpack, 0)

    settle(half, True)
    settle(1 - half, False)

    def multiply(s):
        for m, ref in enumerate((wd, wt)):
            lo, hi, _ = models[m]
            for n in range(CW // 256):
                at = pl.multiple_of(s * CW + n * 256, 256)
                out = lax.dot_general(
                    xn[:, lo:hi], ref[pl.ds(at, 256), :], (((1,), (1,)), ((), ())),
                    preferred_element_type=F32,
                )
                col = m * CW + n * 256
                for blk in range(ROWS // BLOCK):
                    row = (blk // 2) % 2 * BLOCK
                    pb[s, blk % 2, 1 - blk // 4, row : row + BLOCK, col : col + 256] = out[
                        blk * BLOCK : (blk + 1) * BLOCK
                    ]

    def d2_copy(j):
        return remote(pb.at[j, 1 - core], pr.at[j], d2_send.at[j], d2_recv.at[j], v, mate)

    def chain_to(d):
        return (chip + 2 * d - 1) * 2 + core

    def chunk_copy(d, j):
        return remote(sb.at[d, j], rb.at[d, j], c_send.at[d, j], c_recv.at[d, j], v, chain_to(d))

    def scale_copy(d, j):
        return remote(qs.at[d, j], qr.at[d, j], q_send.at[d, j], q_recv.at[d, j], v, chain_to(d))

    groups = CW // 128

    def cut(m, g):
        at = m * CW + g * 128
        return slice(at, at + 128)

    near_end = chip // 2
    depth = chip + near_end * (CHAIN - 1 - 2 * chip)

    def chain(ends_near, s):
        d = near_end if ends_near else 1 - near_end
        pos = (CHAIN - 1) - depth if ends_near else depth
        j = s - LAG - pos * HOP

        @pl.when((j >= 0) & (j < CHUNKS))
        def _():
            def local_sum(m):
                return [
                    pb[j, core, d, :, cut(m, g)] + pr[j, d, :, cut(m, g)] for g in range(groups)
                ]

            def wait_received():
                chunk_copy(d, j).wait_recv()
                scale_copy(d, j).wait_recv()

            def with_received(m):
                unit = qr[d, j]
                return [
                    part + rb[d, j, :, cut(m, g)].astype(F32) * unit
                    for g, part in enumerate(local_sum(m))
                ]

            def code(parts):
                top = functools.reduce(jnp.maximum, [jnp.abs(p) for p in sum(parts, [])])
                top = jnp.maximum(jnp.max(top, axis=0, keepdims=True), 1e-30)
                up = LEVELS / top
                qs[d, j] = top * (1.0 / LEVELS)
                for m in range(2):
                    for g, part in enumerate(parts[m]):
                        sb[d, j, :, cut(m, g)] = (
                            jnp.round(part * up).astype(jnp.int32).astype(jnp.int16)
                        )

            def send():
                scale_copy(d, j).start()
                chunk_copy(d, j).start()

            def first():
                code([local_sum(m) for m in range(2)])
                send()

            def middle():
                wait_received()
                code([with_received(m) for m in range(2)])
                send()

            def last():
                wait_received()
                bits, tok = bt[0], bt[1]
                for m in range(2):
                    logits = with_received(m)
                    high, summed, picked = st[m, 0], st[m, 1], st[m, 2]
                    masked, keeps = [], []
                    for g in range(groups):
                        off = pl.ds(pl.multiple_of(j * CW + g * 128, 128), 128)
                        chosen = colid[:, off] == tok
                        keep = ((bits >> cls[:, off]) & 1 == 1) | chosen
                        picked = picked + jnp.where(chosen, logits[g], 0.0)
                        masked.append(jnp.where(keep, logits[g], NEG))
                        keeps.append(keep)
                    top = functools.reduce(jnp.maximum, masked, high)
                    summed = summed * jnp.exp(high - top)
                    for g in range(groups):
                        summed = summed + jnp.where(keeps[g], jnp.exp(masked[g] - top), 0.0)
                    st[m, 0] = top
                    st[m, 1] = summed
                    st[m, 2] = picked

            pl.when(depth == 1)(middle)
            pl.when(depth == 0)(last if ends_near else first)

    def slot(s, carry):
        @pl.when(s < CHUNKS)
        def _():
            multiply(s)
            d2_copy(s).start()

        late = s - LAG

        @pl.when((late >= 0) & (late < CHUNKS))
        def _():
            d2_copy(late).wait_recv()

        chain(False, s)
        chain(True, s)
        return carry

    lax.fori_loop(0, CHUNKS + LAG + (CHAIN - 1) * HOP, slot, 0)

    owner = (chip == 0) | (chip == CHAIN - 1)
    lane1 = lax.broadcasted_iota(jnp.int32, (1, 128), 1)

    def merge(rows):
        total = jnp.sum(rows, axis=0, keepdims=True)
        top = jnp.max(rows, axis=0, keepdims=True)
        lse = top + jnp.log(jnp.sum(jnp.exp(rows - top), axis=0, keepdims=True))
        return jnp.where(lane1 < 64, lse, total)

    def fin_copy(t):
        return remote(
            grow.at[0], gall.at[place], fin_send.at[t], fin_recv.at[place],
            half * PLANE + (place + t) % PLANE, b,
        )

    def z_copy(n):
        hh = (half + n % 2) % 2
        target = (1 - chip // 2) * 2 + n // 2
        return remote(
            zrow.at[0], zall.at[half], z_send.at[n], z_recv.at[half],
            hh * PLANE + place, target * 2 + core,
        )

    def z_arrived(hh):
        remote(zrow.at[0], zall.at[hh], z_send.at[0], z_recv.at[hh], v, b).wait_recv()

    def drain():
        pair_copy().wait_send()

        def drain_gather(t, carry):
            sum_copy(t).wait_send()
            near_copy(t).wait_send()
            far_copy(t).wait_send()
            return carry

        lax.fori_loop(1, PLANE, drain_gather, 0)

        def drain_chunks(j, carry):
            d2_copy(j).wait_send()
            return carry

        lax.fori_loop(0, CHUNKS, drain_chunks, 0)
        for d in range(2):
            pos = chip if d else (CHAIN - 1) - chip

            @pl.when(pos < CHAIN - 1)
            def _():
                def drain_chain(j, carry):
                    chunk_copy(d, j).wait_send()
                    scale_copy(d, j).wait_send()
                    return carry

                lax.fori_loop(0, CHUNKS, drain_chain, 0)

    @pl.when(owner)
    def _():
        total = jnp.zeros((MINE, 128), F32)
        for m in range(2):
            high, summed, picked = (st[m, n] for n in range(3))
            top = jnp.max(high, axis=1, keepdims=True)
            mass = jnp.sum(summed * jnp.exp(high - top), axis=1, keepdims=True)
            lse = jnp.where(mass > 0.0, top + jnp.log(jnp.maximum(mass, 1e-37)), NEG)
            pick = jnp.sum(picked, axis=1, keepdims=True)
            total = total + jnp.where(lane == sub + m * 32, lse, 0.0)
            total = total + jnp.where(lane == sub + m * 32 + 64, pick, 0.0)
        row = jnp.sum(total, axis=0, keepdims=True)
        grow[0] = row
        gall[place] = row

        for t in AWAY:
            fin_copy(t).start()
        drain()

        def wait(t, carry):
            n = (place + t) % PLANE
            remote(grow.at[0], gall.at[n], fin_send.at[0], fin_recv.at[n], v, b).wait_recv()
            return carry

        lax.fori_loop(1, PLANE, wait, 0)
        row = merge(gall[...].reshape(PLANE, 128))
        zrow[0] = row
        for n in range(4):
            z_copy(n).start()

        def drain_final(t, carry):
            fin_copy(t).wait_send()
            return carry

        lax.fori_loop(1, PLANE, drain_final, 0)
        for n in range(4):
            z_copy(n).wait_send()

    @pl.when(jnp.logical_not(owner))
    def _():
        drain()

    z_arrived(0)
    z_arrived(1)
    row = merge(zall[...].reshape(2, 128))
    for n in range(4):
        out_ref[n : n + 1, :] = jnp.where(
            chip % 2 == 0, row[:, n * 32 : n * 32 + 16], row[:, n * 32 + 16 : n * 32 + 32]
        )


def shards(
    draft_hidden, target_hidden, draft_gain, target_gain, draft_head, target_head,
    token_class, grammar_bits, draft_tokens,
):
    kd, width = draft_head.shape
    kt = target_head.shape[0]
    kk = kd + kt
    vmem, dma = pltpu.VMEM, pltpu.SemaphoreType.DMA
    i32, i16 = jnp.int32, jnp.int16
    scratch = [
        vmem((SHARE, kk), BF16),
        vmem((SHARE, kk), BF16),
        vmem((1, kk), F32),
        vmem((LINE, 1, 128), F32),
        vmem((2 * PLANE, SHARE, kk), BF16),
        vmem((CHUNKS * CW, kd), BF16),
        vmem((CHUNKS * CW, kt), BF16),
        vmem((1, width), i32),
        vmem((1, CHUNKS * CW), i32),
        vmem((1, CHUNKS * CW), i32),
        pltpu.SMEM((ROWS,), i32),
        pltpu.SMEM((ROWS,), i32),
        vmem((4, BLOCK, kk), F32),
        vmem((ROWS, kk), BF16),
        vmem((CHUNKS, 2, 2, MINE, 2 * CW), F32),
        vmem((CHUNKS, 2, MINE, 2 * CW), F32),
        vmem((2, CHUNKS, MINE, 2 * CW), i16),
        vmem((2, CHUNKS, MINE, 2 * CW), i16),
        vmem((2, CHUNKS, 1, 128), F32),
        vmem((2, CHUNKS, 1, 128), F32),
        vmem((2, MINE, 128), i32),
        vmem((2, 3, MINE, 128), F32),
        vmem((1, 1, 128), F32),
        vmem((PLANE, 1, 128), F32),
        vmem((1, 1, 128), F32),
        vmem((2, 1, 128), F32),
        dma((7,)),
        dma((2 * pl.cdiv(width, WSPLIT),)),
        dma((LINE,)),
        dma((LINE,)),
        dma((1,)),
        dma((1,)),
        dma((PLANE,)),
        dma((PLANE,)),
        dma((2 * PLANE,)),
        dma((CHUNKS,)),
        dma((CHUNKS,)),
        dma((2, CHUNKS)),
        dma((2, CHUNKS)),
        dma((2, CHUNKS)),
        dma((2, CHUNKS)),
        dma((PLANE,)),
        dma((PLANE,)),
        dma((4,)),
        dma((2,)),
    ]
    parts = pl.pallas_call(
        functools.partial(kernel, (kd, kt, width)),
        out_shape=pltpu.VMEM((4, BLOCK), F32),
        in_specs=[pl.BlockSpec(memory_space=pl.ANY)] * 9,
        out_specs=pl.BlockSpec(memory_space=pltpu.VMEM),
        scratch_shapes=scratch,
        compiler_params=pltpu.CompilerParams(
            collective_id=0, has_side_effects=True, vmem_limit_bytes=62 * 1024 * 1024
        ),
        name="verify",
    )(
        draft_hidden,
        target_hidden,
        draft_gain.reshape(1, kd),
        target_gain.reshape(1, kt),
        draft_head.T,
        target_head.T,
        token_class.reshape(1, width),
        grammar_bits,
        draft_tokens,
    )
    draft_lse, target_lse, draft_pick, target_pick = (parts[n] for n in range(4))
    logprob = target_pick - target_lse
    return logprob - (draft_pick - draft_lse), logprob


def solution(mesh):
    in_specs = (
        P("vocab", "batch"),
        P("vocab", "batch"),
        P("batch"),
        P("batch"),
        P("batch", "vocab"),
        P("batch", "vocab"),
        P("vocab"),
        P(),
        P(),
    )
    out_specs = (P("batch"), P("batch"))
    return jax.shard_map(shards, mesh=mesh, in_specs=in_specs, out_specs=out_specs, check_vma=False)
```
